256 devices in a mesh: dp: 4 (over y), ep: 64 (over z, x, core).
Axes of the slice: x: 4, y: 4, z: 8, core: 2. Of those that a mesh axis runs over, the one named last changes fastest.
Arguments:
- tokens: bfloat16 [24576, 2048], P(('dp', 'ep')), parts along dimension 0, may hold values from -6 to 6
- routes: int32 [24576, 8], P(('dp', 'ep')), parts along dimension 0, may hold values from 0 to 63, all different within a row; in each aligned block of 96 rows (0 to 95, 96 to 191, ...) at most 18 rows name the same one
- combine_weights: bfloat16 [24576, 8], P(('dp', 'ep')), parts along dimension 0, may hold values from 0.049804688 to 1
- w_gate: bfloat16 [64, 2048, 768], P('ep'), may hold values from -0.125 to 0.125
- w_up: bfloat16 [64, 2048, 768], P('ep'), may hold values from -0.125 to 0.125
- w_down: bfloat16 [64, 768, 2048], P('ep'), may hold values from -0.21875 to 0.21875
Outputs:
- mixed: bfloat16 [24576, 2048], P(('dp', 'ep')), parts along dimension 0
The draws below stay inside these ranges and needn't reach their ends.
There are 4 independent parts, one for each index of `dp`. The reference program is written for one: setup_inputs(seed, part) draws one part's arguments, and reference() takes and returns one part's arrays. A program takes and returns all parts, laid end to end along the dimension named above; an argument that names none is the same for every part. Nothing has to cross between parts.
Inputs may be any that keep to these rules, and one draw needn't show every extreme that they name: `routes`: each row names 8 different experts. Among the 96 rows of one device no expert is named by more than 18 rows, a bound that some blocks reach.
All inputs are finite; a program needn't handle non-finite values.
Results may differ from the reference program's by a relative error of at most 0.012.
Values may be sent and summed in bfloat16 or wider, within the bound.
A program may use at most 128 MiB of HBM per device.

```python
import math
import jax
import jax.numpy as jnp
import numpy as np
from jax import lax

D = 2048
FF = 768
TOP = 8
TOK_DEV = 96
EXPERTS = 64
CAP = 18
TOKENS = 6144
N_EP = 64


def shard_levels(key, extent, cuts, smallest, high):
    gain = 1.0
    for dim, shards_of in cuts:
        steps = jax.random.uniform(jax.random.fold_in(jax.random.fold_in(key, 6), dim), (shards_of,), jnp.float32, smallest / len(cuts), high / len(cuts))
        gain = gain * jnp.repeat(jnp.exp(steps), extent[dim] // shards_of).reshape((-1,) + (1,) * (len(extent) - 1 - dim))
    return gain


def routed_block(rng, own, number, rows, count, top, bound, skew):
    ranking = jax.random.permutation(rng, count)
    crowded, ordinary = load_shares(count, rows * top, bound, skew, True), load_shares(count, rows * top, bound, skew, False)
    places = jnp.arange(count)

    def named(tallies, turn):
        used = int((tallies > 0).sum())
        fixed = max(1, used // 4)
        moved = fixed + (places - fixed + turn * (used - fixed)) % max(1, count - fixed)
        return jnp.zeros((count,), jnp.int32).at[ranking[jnp.where(places < fixed, places, moved)]].set(jnp.asarray(tallies, jnp.int32))

    tallies = jnp.where(number % 4 == 0, named(crowded, number // 4), named(ordinary, number - number // 4 - 1))
    mixed = jax.random.permutation(jax.random.fold_in(own, 3), count)
    source_of, sink = mixed[0:count // 2 * 2:2], mixed[1:count // 2 * 2:2]
    slack = jnp.minimum(tallies[source_of] - 1, bound - tallies[sink]) // 2
    slack = jnp.where((source_of == ranking[0]) | (sink == ranking[0]) | (tallies[sink] == 0), 0, jnp.maximum(slack, 0))
    moved = jax.random.randint(jax.random.fold_in(own, 4), (count // 2,), 0, 1 << 20) % (slack + 1)
    tallies = tallies.at[source_of].add(-moved).at[sink].add(moved)
    members = jnp.searchsorted(jnp.cumsum(tallies), jnp.arange(rows * top), side="right").astype(jnp.int32)
    listing = members.reshape(top, rows).T
    listing = listing[jax.random.permutation(jax.random.fold_in(own, 1), rows)]
    turn = jax.random.randint(jax.random.fold_in(own, 2), (rows, 1), 0, top)
    return jnp.take_along_axis(listing, (jnp.arange(top)[None, :] + turn) % top, axis=1)


def load_shares(number_of, total, reach, skew, full):
    loads = [(1 << 20) // math.isqrt(grade ** skew) + 1 for grade in range(1, number_of + 1)]
    largest = reach if full else min(reach, max(-(-total // number_of), total * loads[0] // sum(loads)))
    least = 1 if total - largest >= number_of - 1 else 0
    given, spare = [largest] + [least] * (number_of - 1), total - largest - least * (number_of - 1)
    while spare > 0:
        candidates = [i for i in range(1, number_of) if given[i] < largest] or [i for i in range(1, number_of) if given[i] < reach]
        mass, budget = sum([loads[i] for i in candidates]), spare
        for i in candidates:
            more = min(reach - given[i], max(1, budget * loads[i] // mass), spare)
            given[i] = given[i] + more
            spare = spare - more
    return np.array(given)


def scatter_about(stream_key, extent, spread, limit, pieces=(), held_as=jnp.bfloat16):
    factor_of = shard_levels(stream_key, extent, pieces, -0.22, 0.18) if pieces else 1.0
    values = jax.random.normal(stream_key, extent, jnp.float32) * spread * factor_of
    return jnp.minimum(jnp.maximum(values, -limit), limit).astype(held_as)


def setup_inputs(seed: int = 0, part: int = 0) -> dict:
    key_list = jax.random.split(jax.random.key(seed), 7)
    own_keys = jax.random.split(jax.random.fold_in(key_list[6], part), 7)
    tokens = scatter_about(own_keys[0], (TOKENS, D), 1.0, 6.0, ((0, 64),))
    routes_keys = jax.random.split(jax.random.fold_in(own_keys[1], 1), TOKENS // TOK_DEV)
    routes_turns = jax.random.permutation(jax.random.fold_in(own_keys[1], 3), TOKENS // TOK_DEV)
    routes = jax.vmap(lambda own, number: routed_block(jax.random.fold_in(own_keys[1], 2), own, number, TOK_DEV, EXPERTS, TOP, CAP, 2))(routes_keys, routes_turns).reshape((TOKENS, TOP))
    combine_weights = jnp.clip(0.049804688 + 0.9501953 * jax.random.uniform(own_keys[2], (TOKENS, TOP), jnp.float32) ** shard_levels(own_keys[2], (TOKENS, TOP), ((0, 64),), -0.2, 0.2), 0.049804688, 1.0).astype(jnp.bfloat16)
    w_gate = scatter_about(key_list[3], (EXPERTS, D, FF), D ** -0.5, 0.125, ((0, 64),))
    w_up = scatter_about(key_list[4], (EXPERTS, D, FF), D ** -0.5, 0.125, ((0, 64),))
    w_down = scatter_about(key_list[5], (EXPERTS, FF, D), FF ** -0.5, 0.21875, ((0, 64),))
    return {"tokens": tokens, "routes": routes, "combine_weights": combine_weights, "w_gate": w_gate, "w_up": w_up, "w_down": w_down}


def expert_ffn(rows, row_weight, gate_matrix, upward_matrix, down_matrix):
    gate = jnp.dot(rows, gate_matrix, preferred_element_type=jnp.float32)
    upward = jnp.dot(rows, upward_matrix, preferred_element_type=jnp.float32)
    hidden = (jax.nn.silu(gate) * upward).astype(jnp.bfloat16)
    result = jnp.dot(hidden, down_matrix, preferred_element_type=jnp.float32)
    return (result * row_weight.astype(jnp.float32)[:, None]).astype(jnp.bfloat16)


def reference(tokens, routes, combine_weights, w_gate, w_up, w_down):
    pairs = TOKENS * TOP
    flat_routes = routes.reshape(-1)
    flat_weights = combine_weights.reshape(-1)
    room = N_EP * CAP

    def one_expert(total, expert):
        pair_index = jnp.nonzero(flat_routes == expert, size=room, fill_value=pairs)[0].astype(jnp.int32)
        token_index = (pair_index // TOP).astype(jnp.int32)
        rows = jnp.take(tokens, token_index, axis=0, mode="fill", fill_value=0)
        row_weight = jnp.take(flat_weights, pair_index, mode="fill", fill_value=0)
        result = expert_ffn(rows, row_weight, w_gate[expert], w_up[expert], w_down[expert])
        total = total.at[token_index].add(result.astype(jnp.float32), mode="drop")
        return total, None

    start = jnp.zeros((TOKENS, D), jnp.float32)
    total, unused = lax.scan(one_expert, start, jnp.arange(EXPERTS, dtype=jnp.int32))
    return total.astype(jnp.bfloat16)
```

```python
import jax
import jax.numpy as jnp
from jax import lax
from jax.experimental import pallas as pl
from jax.experimental.pallas import tpu as pltpu
from jax.sharding import PartitionSpec as P

MESH = pl.DeviceIdType.MESH
F32, BF16 = jnp.float32, jnp.bfloat16

NZ, NR = 8, 8
TOK, DIM, HID = 96, 2048, 768
MAIN = 16
BLK = NR * MAIN
OVF = NZ * BLK
ROWS = OVF + BLK
HALF = TOK // 2
COLS = 512

OFFSET = (0, -1, 1, -2, 2, -3, 3, 4)
STEPS = ((0, 128), (128, 256), (384, 256), (640, 256), (896, 256))


def one_hot_dot(a, b):
    return jnp.dot(a, b, preferred_element_type=F32)


def kernel(
    tokens, meta, w_gate, w_up, w_down, out,
    xz, sx, rx, ys, yr, zs, zr, wg, wu, wd, hid, pm, pmr, cm,
    local_sem, zsend, zrecv, msend, mrecv, xsend, xrecv, ysend, yrecv, rsend, rrecv,
):
    me = lax.axis_index("ep")
    z, r = me // NR, me % NR

    def at_z(d):
        return {"ep": lax.rem(z + d + NZ, NZ) * NR + r}

    def at_r(i):
        return lax.rem(r + i, NR)

    loads = [
        pltpu.make_async_copy(tokens, xz.at[0], local_sem.at[0]),
        pltpu.make_async_copy(w_gate.at[0], wg, local_sem.at[1]),
        pltpu.make_async_copy(w_up.at[0], wu, local_sem.at[2]),
        pltpu.make_async_copy(w_down.at[0], wd, local_sem.at[3]),
    ]
    for load in loads:
        load.start()

    barrier = pltpu.get_barrier_semaphore()
    for d in range(1, NZ):
        pl.semaphore_signal(barrier, inc=1, device_id=at_z(d), device_id_type=MESH)
    for i in range(1, NR):
        pl.semaphore_signal(barrier, inc=1, device_id={"ep": z * NR + at_r(i)}, device_id_type=MESH)

    expert = lax.broadcasted_iota(jnp.int32, (NZ * NR, 128), 0).astype(F32)
    named = jnp.zeros((NZ * NR, 128), F32)
    weight = jnp.zeros((NZ * NR, 128), F32)
    for k in range(8):
        hit = meta[k : k + 1, :] == expert
        named = jnp.where(hit, 1.0, named)
        weight = jnp.where(hit, meta[8 + k : 9 + k, :], weight)
    before = (
        lax.broadcasted_iota(jnp.int32, (128, 128), 0) < lax.broadcasted_iota(jnp.int32, (128, 128), 1)
    ).astype(F32).astype(BF16)
    place = one_hot_dot(named.astype(BF16), before)
    pm[:, 0:128] = jnp.where(named > 0.0, place, -1.0)
    pm[:, 128:256] = weight

    pl.semaphore_wait(barrier, NZ - 1 + NR - 1)

    def ring(k, src, dst, sem, rows=slice(0, TOK)):
        lo, n = rows.start, rows.stop - rows.start
        return pltpu.make_async_remote_copy(
            src_ref=xz.at[src, pl.ds(lo, n)], dst_ref=xz.at[dst, pl.ds(lo, n)],
            send_sem=zsend.at[sem], recv_sem=zrecv.at[sem], device_id=at_z(k), device_id_type=MESH,
        )

    loads[0].wait()
    up = [ring(1, 0, 1, 0), ring(1, 1, 3, 2), ring(1, 3, 5, 4), ring(1, 5, 7, 6, slice(0, HALF))]
    down = [ring(-1, 0, 2, 1), ring(-1, 2, 4, 3), ring(-1, 4, 6, 5), ring(-1, 6, 7, 7, slice(HALF, TOK))]
    metas = []
    for j in range(1, NZ):
        d = -OFFSET[j]
        metas.append(
            pltpu.make_async_remote_copy(
                src_ref=pm.at[pl.ds(pl.multiple_of(lax.rem(z + d + NZ, NZ) * NR, NR), NR)],
                dst_ref=pmr.at[j], send_sem=msend.at[j], recv_sem=mrecv.at[j],
                device_id=at_z(d), device_id_type=MESH,
            )
        )
    for copy in metas:
        copy.start()
    up[0].start()
    down[0].start()
    pmr[0] = pm[pl.ds(pl.multiple_of(z * NR, NR), NR), :]

    row = lax.broadcasted_iota(jnp.int32, (BLK, 128), 0)
    spread = (
        lax.broadcasted_iota(jnp.int32, (BLK, NR), 0) // MAIN == lax.broadcasted_iota(jnp.int32, (BLK, NR), 1)
    ).astype(F32).astype(BF16)

    def selections(j):
        place_j = one_hot_dot(spread, pmr[j, :, 0:128].astype(BF16))
        weight_j = one_hot_dot(spread, pmr[j, :, 128:256].astype(BF16))
        main = place_j == (row % MAIN).astype(F32)
        extra = (place_j == (MAIN + row % 2).astype(F32)) & (row % MAIN // 2 == j)
        cm[j, :, 0:BLK] = jnp.transpose(jnp.where(main, weight_j, 0.0))[0:TOK].astype(BF16)
        cm[j, :, BLK : 2 * BLK] = jnp.transpose(jnp.where(extra, weight_j, 0.0))[0:TOK].astype(BF16)
        return (
            jnp.where(main, 1.0, 0.0).astype(BF16)[:, 0:TOK],
            jnp.where(extra, 1.0, 0.0).astype(BF16)[:, 0:TOK],
        )

    mine = pl.multiple_of(r * MAIN, MAIN)

    def exchange(src, dst, first, n, send_sem, recv_sem):
        for lo in range(first, first + n, BLK):
            dst[pl.ds(lo + mine, MAIN), :] = src[pl.ds(lo + mine, MAIN), :]
        for i in range(1, NR):
            to = at_r(i)
            theirs = pl.multiple_of(to * MAIN, MAIN)
            for lo in range(first, first + n, BLK):
                pltpu.make_async_remote_copy(
                    src_ref=src.at[pl.ds(lo + theirs, MAIN)], dst_ref=dst.at[pl.ds(lo + mine, MAIN)],
                    send_sem=send_sem, recv_sem=recv_sem,
                    device_id={"ep": z * NR + to}, device_id_type=MESH,
                ).start()

    def drained(ref, n, sem):
        part = ref.at[pl.ds(0, n // BLK * (BLK - MAIN))]
        pltpu.make_async_copy(part, part, sem).wait()

    extras = []

    def gather(j):
        main, extra = selections(j)
        extras.append(extra)
        for c in range(0, DIM, COLS):
            sx[j * BLK : (j + 1) * BLK, c : c + COLS] = one_hot_dot(main, xz[j, :, c : c + COLS]).astype(BF16)

    def gather_overflow():
        for c in range(0, DIM, COLS):
            total = one_hot_dot(extras[0], xz[0, :, c : c + COLS])
            for j in range(1, NZ):
                total += one_hot_dot(extras[j], xz[j, :, c : c + COLS])
            sx[OVF:ROWS, c : c + COLS] = total.astype(BF16)

    def experts(step):
        first, n = STEPS[step]
        drained(rx, n, xrecv.at[step])

        def hidden(i, carry):
            c = pl.ds(pl.multiple_of(i * 256, 256), 256)
            rows = rx[first : first + n, :]
            gate = jnp.dot(rows, wg[:, c], preferred_element_type=F32)
            upward = jnp.dot(rows, wu[:, c], preferred_element_type=F32)
            hid[0:n, c] = (gate / (1.0 + jnp.exp(-gate)) * upward).astype(BF16)
            return carry

        def result(i, carry):
            c = pl.ds(pl.multiple_of(i * 256, 256), 256)
            ys[first : first + n, c] = jnp.dot(hid[0:n, :], wd[:, c], preferred_element_type=F32).astype(BF16)
            return carry

        lax.fori_loop(0, HID // 256, hidden, 0)
        lax.fori_loop(0, DIM // 256, result, 0)

    def dispatch(step):
        first, n = STEPS[step]
        exchange(sx, rx, first, n, xsend.at[step], xrecv.at[step])

    def give_back(step):
        first, n = STEPS[step]
        exchange(ys, yr, first, n, ysend.at[step], yrecv.at[step])

    gather(0)
    dispatch(0)
    for load in loads[1:]:
        load.wait()

    for k in (1, 2, 3):
        up[k - 1].wait_recv()
        up[k].start()
        down[k - 1].wait_recv()
        down[k].start()
        for j in (2 * k - 1, 2 * k):
            metas[j - 1].wait_recv()
            gather(j)
        dispatch(k)
        experts(k - 1)
    up[3].wait_recv()
    down[3].wait_recv()
    metas[6].wait_recv()
    gather(7)
    gather_overflow()
    dispatch(4)
    experts(3)
    give_back(3)
    experts(4)
    for step in (4, 2, 1, 0):
        give_back(step)

    def combine(j, c):
        return one_hot_dot(cm[j, :, 0:BLK], yr[j * BLK : (j + 1) * BLK, c : c + COLS]) + one_hot_dot(
            cm[j, :, BLK : 2 * BLK], yr[OVF:ROWS, c : c + COLS]
        )

    def homeward(way, m, lo, n):
        return pltpu.make_async_remote_copy(
            src_ref=zs.at[way, m, pl.ds(lo, n)], dst_ref=zr.at[way, m, pl.ds(lo, n)],
            send_sem=rsend.at[way, m], recv_sem=rrecv.at[way, m],
            device_id=at_z(1 - 2 * way), device_id_type=MESH,
        )

    spans = ((0, HALF), (HALF, HALF))
    home = [[homeward(way, 0, *spans[way])] + [homeward(way, m, 0, TOK) for m in (1, 2, 3)] for way in (0, 1)]

    drained(yr, STEPS[4][1], yrecv.at[4])
    for c in range(0, DIM, COLS):
        part = combine(7, c).astype(BF16)
        zs[0, 0, 0:HALF, c : c + COLS] = part[0:HALF]
        zs[1, 0, HALF:TOK, c : c + COLS] = part[HALF:TOK]
    for way in (0, 1):
        home[way][0].start()
    for m in (1, 2, 3):
        step = 4 - m
        drained(yr, STEPS[step][1], yrecv.at[step])
        for way, j in ((0, 2 * step), (1, 2 * step - 1)):
            home[way][m - 1].wait_recv()
            for c in range(0, DIM, COLS):
                part = combine(j, c)
                if m == 1:
                    lo, n = spans[way]
                    came = zr[way, 0, lo : lo + n, c : c + COLS].astype(F32)
                    zs[way, 1, lo : lo + n, c : c + COLS] = (part[lo : lo + n] + came).astype(BF16)
                    lo = HALF - lo
                    zs[way, 1, lo : lo + n, c : c + COLS] = part[lo : lo + n].astype(BF16)
                else:
                    came = zr[way, m - 1, :, c : c + COLS].astype(F32)
                    zs[way, m, :, c : c + COLS] = (part + came).astype(BF16)
            home[way][m].start()
    drained(yr, STEPS[0][1], yrecv.at[0])
    home[0][3].wait_recv()
    home[1][3].wait_recv()
    for c in range(0, DIM, COLS):
        total = combine(0, c) + zr[0, 3, :, c : c + COLS].astype(F32) + zr[1, 3, :, c : c + COLS].astype(F32)
        out[:, c : c + COLS] = total.astype(BF16)

    for copy in up + down + metas + home[0] + home[1]:
        copy.wait_send()
    for step in range(5):
        drained(sx, STEPS[step][1], xsend.at[step])
        drained(ys, STEPS[step][1], ysend.at[step])


def local(tokens, routes, combine_weights, w_gate, w_up, w_down):
    meta = jnp.concatenate([routes.T.astype(F32), combine_weights.T.astype(F32)], axis=0)
    meta = jnp.pad(meta, ((0, 0), (0, 128 - TOK)), constant_values=-1.0)
    anywhere = pl.BlockSpec(memory_space=pl.ANY)
    vmem = pl.BlockSpec(memory_space=pltpu.VMEM)
    dma = pltpu.SemaphoreType.DMA
    return pl.pallas_call(
        kernel,
        name="routed_experts",
        out_shape=jax.ShapeDtypeStruct((TOK, DIM), BF16),
        in_specs=[anywhere, vmem, anywhere, anywhere, anywhere],
        out_specs=vmem,
        scratch_shapes=[
            pltpu.VMEM((NZ, TOK, DIM), BF16),
            pltpu.VMEM((ROWS, DIM), BF16),
            pltpu.VMEM((ROWS, DIM), BF16),
            pltpu.VMEM((ROWS, DIM), BF16),
            pltpu.VMEM((ROWS, DIM), BF16),
            pltpu.VMEM((2, 4, TOK, DIM), BF16),
            pltpu.VMEM((2, 4, TOK, DIM), BF16),
            pltpu.VMEM((DIM, HID), BF16),
            pltpu.VMEM((DIM, HID), BF16),
            pltpu.VMEM((HID, DIM), BF16),
            pltpu.VMEM((256, HID), BF16),
            pltpu.VMEM((NZ * NR, 256), F32),
            pltpu.VMEM((NZ, NR, 256), F32),
            pltpu.VMEM((NZ, TOK, 2 * BLK), BF16),
            dma((4,)), dma((8,)), dma((8,)), dma((8,)), dma((8,)),
            dma((5,)), dma((5,)), dma((5,)), dma((5,)), dma((2, 4)), dma((2, 4)),
        ],
        compiler_params=pltpu.CompilerParams(
            collective_id=0, has_side_effects=True, vmem_limit_bytes=67_043_328
        ),
    )(tokens, meta, w_gate, w_up, w_down)


def solution(mesh):
    in_specs = (
        P(("dp", "ep"), None), P(("dp", "ep"), None), P(("dp", "ep"), None),
        P("ep", None, None), P("ep", None, None), P("ep", None, None),
    )
    return jax.shard_map(
        local, mesh=mesh, in_specs=in_specs, out_specs=P(("dp", "ep"), None), check_vma=False
    )
```

```python
import jax
import jax.numpy as jnp
from jax import lax
from jax.experimental import pallas as pl
from jax.experimental.pallas import tpu as pltpu
from jax.sharding import PartitionSpec as P

MESH = pl.DeviceIdType.MESH
F32, BF16 = jnp.float32, jnp.bfloat16

NZ, NR = 8, 8
TOK, DIM, HID = 96, 2048, 768
MAIN = 16
BLK = NR * MAIN
OVF = NZ * BLK
ROWS = OVF + BLK
HALF = TOK // 2
PARTS = 4
COLS = DIM // PARTS

OFFSET = (0, -1, 1, -2, 2, -3, 3, 4)
STEPS = ((0, 128), (128, 256), (384, 256), (640, 256), (896, 256))


def one_hot_dot(a, b):
    return jnp.dot(a, b, preferred_element_type=F32)


def kernel(
    tokens, routes, weights, w_gate, w_up, w_down, out,
    xz, sx, rx, ys, yr, zs, zr, wg, wu, wd, hid, square, meta, cm,
    local_sem, zsend, zrecv, msend, mrecv, xsend, xrecv, ysend, yrecv, rsend, rrecv,
):
    me = lax.axis_index("ep")
    z, r = me // NR, me % NR

    def at_z(d):
        return {"ep": lax.rem(z + d + NZ, NZ) * NR + r}

    def at_r(i):
        return lax.rem(r + i, NR)

    loads = [
        pltpu.make_async_copy(tokens, xz.at[0], local_sem.at[0]),
        pltpu.make_async_copy(w_gate.at[0], wg, local_sem.at[1]),
        pltpu.make_async_copy(w_up.at[0], wu, local_sem.at[2]),
        pltpu.make_async_copy(w_down.at[0], wd, local_sem.at[3]),
    ]
    for load in loads:
        load.start()

    barrier = pltpu.get_barrier_semaphore()
    for d in (-1, 1):
        pl.semaphore_signal(barrier, inc=1, device_id=at_z(d), device_id_type=MESH)
    for i in range(1, NR):
        pl.semaphore_signal(barrier, inc=1, device_id={"ep": z * NR + at_r(i)}, device_id_type=MESH)

    square[...] = jnp.full((128, 128), -1.0, F32)
    square[0:TOK, 0:8] = routes[...].astype(F32)
    square[0:TOK, 8:16] = weights[...].astype(F32)
    meta[0] = jnp.transpose(square[...])[0:16]

    pl.semaphore_wait(barrier, 2 + NR - 1)

    def ring(k, src, dst, sem, rows=slice(0, TOK)):
        lo, n = rows.start, rows.stop - rows.start
        return [
            pltpu.make_async_remote_copy(
                src_ref=xz.at[src, pl.ds(lo, n), pl.ds(h * COLS, COLS)],
                dst_ref=xz.at[dst, pl.ds(lo, n), pl.ds(h * COLS, COLS)],
                send_sem=zsend.at[sem, h], recv_sem=zrecv.at[sem, h], device_id=at_z(k), device_id_type=MESH,
            )
            for h in range(PARTS)
        ]

    def table(k, src, dst):
        return pltpu.make_async_remote_copy(
            src_ref=meta.at[src], dst_ref=meta.at[dst], send_sem=msend.at[dst], recv_sem=mrecv.at[dst],
            device_id=at_z(k), device_id_type=MESH,
        )

    up = [ring(1, 0, 1, 0), ring(1, 1, 3, 2), ring(1, 3, 5, 4), ring(1, 5, 7, 6, slice(0, HALF))]
    down = [ring(-1, 0, 2, 1), ring(-1, 2, 4, 3), ring(-1, 4, 6, 5), ring(-1, 6, 7, 7, slice(HALF, TOK))]
    metas = [None, table(1, 0, 1), table(-1, 0, 2), table(1, 1, 3), table(-1, 2, 4), table(1, 3, 5), table(-1, 4, 6), table(1, 5, 7)]
    metas[1].start()
    metas[2].start()
    loads[0].wait()
    for h in range(PARTS):
        up[0][h].start()
        down[0][h].start()

    row = lax.broadcasted_iota(jnp.int32, (BLK, 128), 0)
    spread = (
        lax.broadcasted_iota(jnp.int32, (BLK, NR), 0) // MAIN == lax.broadcasted_iota(jnp.int32, (BLK, NR), 1)
    ).astype(F32).astype(BF16)

    before = (
        lax.broadcasted_iota(jnp.int32, (128, 128), 0) < lax.broadcasted_iota(jnp.int32, (128, 128), 1)
    ).astype(F32).astype(BF16)
    expert = (lax.broadcasted_iota(jnp.int32, (NR, 128), 0) + z * NR).astype(F32)

    def selections(j):
        named = jnp.zeros((NR, 128), F32)
        weight = jnp.zeros((NR, 128), F32)
        for k in range(8):
            hit = meta[j, k : k + 1, :] == expert
            named = jnp.where(hit, 1.0, named)
            weight = jnp.where(hit, meta[j, 8 + k : 9 + k, :], weight)
        place = jnp.where(named > 0.0, one_hot_dot(named.astype(BF16), before), -1.0)
        place_j = one_hot_dot(spread, place.astype(BF16))
        weight_j = one_hot_dot(spread, weight.astype(BF16))
        main = place_j == (row % MAIN).astype(F32)
        extra = (place_j == (MAIN + row % 2).astype(F32)) & (row % MAIN // 2 == j)
        cm[j, :, 0:BLK] = jnp.transpose(jnp.where(main, weight_j, 0.0))[0:TOK].astype(BF16)
        cm[j, :, BLK : 2 * BLK] = jnp.transpose(jnp.where(extra, weight_j, 0.0))[0:TOK].astype(BF16)
        return (
            jnp.where(main, 1.0, 0.0).astype(BF16)[:, 0:TOK],
            jnp.where(extra, 1.0, 0.0).astype(BF16)[:, 0:TOK],
        )

    mine = pl.multiple_of(r * MAIN, MAIN)

    def exchange(src, dst, first, n, send_sem, recv_sem, c, w):
        for lo in range(first, first + n, BLK):
            dst[pl.ds(lo + mine, MAIN), c : c + w] = src[pl.ds(lo + mine, MAIN), c : c + w]
        for i in range(1, NR):
            to = at_r(i)
            theirs = pl.multiple_of(to * MAIN, MAIN)
            for lo in range(first, first + n, BLK):
                pltpu.make_async_remote_copy(
                    src_ref=src.at[pl.ds(lo + theirs, MAIN), pl.ds(c, w)],
                    dst_ref=dst.at[pl.ds(lo + mine, MAIN), pl.ds(c, w)],
                    send_sem=send_sem, recv_sem=recv_sem,
                    device_id={"ep": z * NR + to}, device_id_type=MESH,
                ).start()

    def drained(ref, n, sem, w=DIM):
        part = ref.at[pl.ds(0, n // BLK * (BLK - MAIN)), pl.ds(0, w)]
        pltpu.make_async_copy(part, part, sem).wait()

    extras = []

    picks = {}

    def gather(j, h):
        if h == 0:
            picks[j], extra = selections(j)
            extras.append(extra)
        c = h * COLS
        sx[j * BLK : (j + 1) * BLK, c : c + COLS] = one_hot_dot(picks[j], xz[j, :, c : c + COLS]).astype(BF16)

    def gather_overflow():
        for c in range(0, DIM, COLS):
            total = one_hot_dot(extras[0], xz[0, :, c : c + COLS])
            for j in range(1, NZ):
                total += one_hot_dot(extras[j], xz[j, :, c : c + COLS])
            sx[OVF:ROWS, c : c + COLS] = total.astype(BF16)

    def experts(step):
        first, n = STEPS[step]
        drained(rx, n, xrecv.at[step])

        def hidden(i, carry):
            c = pl.ds(pl.multiple_of(i * 256, 256), 256)
            rows = rx[first : first + n, :]
            gate = jnp.dot(rows, wg[:, c], preferred_element_type=F32)
            upward = jnp.dot(rows, wu[:, c], preferred_element_type=F32)
            hid[0:n, c] = (gate / (1.0 + jnp.exp(-gate)) * upward).astype(BF16)
            return carry

        def result(i, carry):
            c = pl.ds(pl.multiple_of(i * 256, 256), 256)
            ys[first : first + n, c] = jnp.dot(hid[0:n, :], wd[:, c], preferred_element_type=F32).astype(BF16)
            return carry

        lax.fori_loop(0, HID // 256, hidden, 0)
        lax.fori_loop(0, DIM // 256, result, 0)

    def dispatch(step, c=0, w=DIM):
        first, n = STEPS[step]
        exchange(sx, rx, first, n, xsend.at[step], xrecv.at[step], c, w)

    def give_back(step):
        first, n = STEPS[step]
        for h in range(PARTS):
            exchange(ys, yr, first, n, ysend.at[step], yrecv.at[step, h], h * COLS, COLS)

    def arrive(k):
        for j in (2 * k - 1, 2 * k):
            metas[j].wait_recv()
            if j + 2 < NZ:
                metas[j + 2].start()
        for h in range(PARTS):
            up[k - 1][h].wait_recv()
            up[k][h].start()
            down[k - 1][h].wait_recv()
            down[k][h].start()
            gather(2 * k - 1, h)
            gather(2 * k, h)
            if k == 1:
                dispatch(1, h * COLS, COLS)
        if k > 1:
            dispatch(k)

    for h in range(PARTS):
        gather(0, h)
        dispatch(0, h * COLS, COLS)
    for load in loads[1:]:
        load.wait()
    arrive(1)
    experts(0)
    arrive(2)
    experts(1)
    arrive(3)
    metas[7].wait_recv()
    for h in range(PARTS):
        up[3][h].wait_recv()
        down[3][h].wait_recv()
        gather(7, h)
    gather_overflow()
    dispatch(4)
    experts(2)
    experts(3)
    give_back(3)
    experts(4)
    for step in (4, 2, 1, 0):
        give_back(step)

    def combine(j, c):
        return one_hot_dot(cm[j, :, 0:BLK], yr[j * BLK : (j + 1) * BLK, c : c + COLS]) + one_hot_dot(
            cm[j, :, BLK : 2 * BLK], yr[OVF:ROWS, c : c + COLS]
        )

    def homeward(way, m, lo, n):
        return [
            pltpu.make_async_remote_copy(
                src_ref=zs.at[way, m, pl.ds(lo, n), pl.ds(h * COLS, COLS)],
                dst_ref=zr.at[way, m, pl.ds(lo, n), pl.ds(h * COLS, COLS)],
                send_sem=rsend.at[way, m, h], recv_sem=rrecv.at[way, m, h],
                device_id=at_z(1 - 2 * way), device_id_type=MESH,
            )
            for h in range(PARTS)
        ]

    spans = ((0, HALF), (HALF, HALF))
    home = [[homeward(way, 0, *spans[way])] + [homeward(way, m, 0, TOK) for m in (1, 2, 3)] for way in (0, 1)]

    for h in range(PARTS):
        c = h * COLS
        drained(yr, STEPS[4][1], yrecv.at[4, h], COLS)
        part = combine(7, c).astype(BF16)
        for way in (0, 1):
            lo, n = spans[way]
            zs[way, 0, lo : lo + n, c : c + COLS] = part[lo : lo + n]
            home[way][0][h].start()
    for m in (1, 2, 3):
        step = 4 - m
        for h in range(PARTS):
            c = h * COLS
            drained(yr, STEPS[step][1], yrecv.at[step, h], COLS)
            for way, j in ((0, 2 * step), (1, 2 * step - 1)):
                part = combine(j, c)
                home[way][m - 1][h].wait_recv()
                if m == 1:
                    lo, n = spans[way]
                    came = zr[way, 0, lo : lo + n, c : c + COLS].astype(F32)
                    zs[way, 1, lo : lo + n, c : c + COLS] = (part[lo : lo + n] + came).astype(BF16)
                    lo = HALF - lo
                    zs[way, 1, lo : lo + n, c : c + COLS] = part[lo : lo + n].astype(BF16)
                else:
                    came = zr[way, m - 1, :, c : c + COLS].astype(F32)
                    zs[way, m, :, c : c + COLS] = (part + came).astype(BF16)
                home[way][m][h].start()
    for h in range(PARTS):
        c = h * COLS
        drained(yr, STEPS[0][1], yrecv.at[0, h], COLS)
        part = combine(0, c)
        home[0][3][h].wait_recv()
        home[1][3][h].wait_recv()
        total = part + zr[0, 3, :, c : c + COLS].astype(F32) + zr[1, 3, :, c : c + COLS].astype(F32)
        out[:, c : c + COLS] = total.astype(BF16)

    for message in up + down + home[0] + home[1]:
        for copy in message:
            copy.wait_send()
    for copy in metas[1:]:
        copy.wait_send()
    for step in range(5):
        drained(sx, STEPS[step][1], xsend.at[step])
        drained(ys, STEPS[step][1], ysend.at[step])


def local(tokens, routes, combine_weights, w_gate, w_up, w_down):
    anywhere = pl.BlockSpec(memory_space=pl.ANY)
    vmem = pl.BlockSpec(memory_space=pltpu.VMEM)
    dma = pltpu.SemaphoreType.DMA
    return pl.pallas_call(
        kernel,
        name="routed_experts",
        out_shape=jax.ShapeDtypeStruct((TOK, DIM), BF16),
        in_specs=[anywhere, vmem, vmem, anywhere, anywhere, anywhere],
        out_specs=vmem,
        scratch_shapes=[
            pltpu.VMEM((NZ, TOK, DIM), BF16),
            pltpu.VMEM((ROWS, DIM), BF16),
            pltpu.VMEM((ROWS, DIM), BF16),
            pltpu.VMEM((ROWS, DIM), BF16),
            pltpu.VMEM((ROWS, DIM), BF16),
            pltpu.VMEM((2, 4, TOK, DIM), BF16),
            pltpu.VMEM((2, 4, TOK, DIM), BF16),
            pltpu.VMEM((DIM, HID), BF16),
            pltpu.VMEM((DIM, HID), BF16),
            pltpu.VMEM((HID, DIM), BF16),
            pltpu.VMEM((256, HID), BF16),
            pltpu.VMEM((128, 128), F32),
            pltpu.VMEM((NZ, 16, 128), F32),
            pltpu.VMEM((NZ, TOK, 2 * BLK), BF16),
            dma((4,)), dma((8, PARTS)), dma((8, PARTS)), dma((8,)), dma((8,)),
            dma((5,)), dma((5,)), dma((5,)), dma((5, PARTS)), dma((2, 4, PARTS)), dma((2, 4, PARTS)),
        ],
        compiler_params=pltpu.CompilerParams(
            collective_id=0, has_side_effects=True, vmem_limit_bytes=67_043_328
        ),
    )(tokens, routes, combine_weights, w_gate, w_up, w_down)


def solution(mesh):
    in_specs = (
        P(("dp", "ep"), None), P(("dp", "ep"), None), P(("dp", "ep"), None),
        P("ep", None, None), P("ep", None, None), P("ep", None, None),
    )
    return jax.shard_map(
        local, mesh=mesh, in_specs=in_specs, out_specs=P(("dp", "ep"), None), check_vma=False
    )
```

```python
import jax
import jax.numpy as jnp
from jax import lax
from jax.experimental import pallas as pl
from jax.experimental.pallas import tpu as pltpu
from jax.sharding import PartitionSpec as P

MESH = pl.DeviceIdType.MESH
F32, BF16 = jnp.float32, jnp.bfloat16

NZ, NX, NR = 8, 4, 8
TOK, DIM, HID = 96, 2048, 768
MAIN = 16
BLK = NR * MAIN
OVF = NZ * BLK
ROWS = OVF + BLK
HALF = TOK // 2
NEAR = 4 * MAIN

PARTS, DUAL = 4, 1
FULL = PARTS - DUAL
COLS = DIM // PARTS
DCOLS = DUAL * COLS
WIDE = DIM + DCOLS
SECOND = tuple(range(PARTS, PARTS + DUAL))
RETURNED = tuple(range(FULL, PARTS)) + tuple(range(FULL))

OFFSET = (0, -1, 1, -2, 2, -3, 3, 4)
SLOTS = ((0,), (1, 2), (3, 4), (5, 6), (7,))


def dot(a, b):
    return jnp.dot(a, b, preferred_element_type=F32)


def iota(shape, axis):
    return lax.broadcasted_iota(jnp.int32, shape, axis)


def kernel(
    tokens, routes, weights, w_gate, w_up, w_down, out,
    xz, sx, rx, ys, yr, so, sn, yo, yn, zs, zr, fs, fr,
    wg, wu, wd, hid, listed, weighed, square, meta, metn, cm, co, cn,
    local_sem, zsend, zrecv, msend, mrecv, nsend, nrecv, dsend, drecv,
    xsend, xrecv, tsend, trecv, osend, orecv, ysend, yrecv, psend, precv, rsend, rrecv, fsend, frecv,
):
    me = lax.axis_index("ep")
    z, r = me // NR, me % NR
    x, c = r // 2, r % 2
    s = 1 - 2 * c

    def at_z(d):
        return {"ep": lax.rem(z + d + NZ, NZ) * NR + r}

    def in_row(other):
        return {"ep": z * NR + other}

    def device(dx, core):
        return lax.rem(x + dx + 2 * NX, NX) * 2 + core

    def tile(row):
        return pl.ds(pl.multiple_of(row, MAIN), MAIN)

    second, host_of = device(s, c), device(-s, c)
    loads = [
        pltpu.make_async_copy(routes, listed, local_sem.at[0]),
        pltpu.make_async_copy(weights, weighed, local_sem.at[1]),
        pltpu.make_async_copy(tokens, xz.at[0, :, pl.ds(0, DIM)], local_sem.at[2]),
        pltpu.make_async_copy(w_gate.at[0], wg, local_sem.at[3]),
        pltpu.make_async_copy(w_up.at[0], wu, local_sem.at[4]),
        pltpu.make_async_copy(w_down.at[0], wd, local_sem.at[5]),
    ]
    barrier = pltpu.get_barrier_semaphore()
    for d in (-1, 1):
        pl.semaphore_signal(barrier, inc=1, device_id=at_z(d), device_id_type=MESH)
    for i in range(1, NR):
        pl.semaphore_signal(barrier, inc=1, device_id=in_row(lax.rem(r + i, NR)), device_id_type=MESH)
    for load in loads:
        load.start()

    square[...] = jnp.full((128, 128), -1.0, F32)
    loads[0].wait()
    square[0:TOK, 0:8] = listed[...].astype(F32)
    loads[1].wait()
    square[0:TOK, 8:16] = weighed[...].astype(F32)
    meta[0] = jnp.transpose(square[...])[0:16]

    def ring(k, src, dst, sem, lo=0, n=TOK):
        return [
            pltpu.make_async_remote_copy(
                src_ref=xz.at[src, pl.ds(lo, n), pl.ds(h * COLS, COLS)],
                dst_ref=xz.at[dst, pl.ds(lo, n), pl.ds(h * COLS, COLS)],
                send_sem=zsend.at[sem, h], recv_sem=zrecv.at[sem, h], device_id=at_z(k), device_id_type=MESH,
            )
            for h in range(PARTS + DUAL)
        ]

    def tables(ref, send, recv):
        return [None] + [
            pltpu.make_async_remote_copy(
                src_ref=ref.at[max(j - 2, 0)], dst_ref=ref.at[j], send_sem=send.at[j], recv_sem=recv.at[j],
                device_id=at_z(1 if j % 2 else -1), device_id_type=MESH,
            )
            for j in range(1, NZ)
        ]

    up = [ring(1, 0, 1, 0), ring(1, 1, 3, 2), ring(1, 3, 5, 4), ring(1, 5, 7, 6, 0, HALF)]
    down = [ring(-1, 0, 2, 1), ring(-1, 2, 4, 3), ring(-1, 4, 6, 5), ring(-1, 6, 7, 7, HALF, HALF)]
    metas, metns = tables(meta, msend, mrecv), tables(metn, nsend, nrecv)
    dense = [
        pltpu.make_async_remote_copy(
            src_ref=xz.at[0, :, pl.ds((FULL + i) * COLS, COLS)], dst_ref=xz.at[0, :, pl.ds((PARTS + i) * COLS, COLS)],
            send_sem=dsend.at[i], recv_sem=drecv.at[i], device_id=in_row(second), device_id_type=MESH,
        )
        for i in range(DUAL)
    ]
    dense_table = pltpu.make_async_remote_copy(
        src_ref=meta.at[0], dst_ref=metn.at[0], send_sem=nsend.at[0], recv_sem=nrecv.at[0],
        device_id=in_row(second), device_id_type=MESH,
    )

    pl.semaphore_wait(barrier, 2 + NR - 1)
    metas[1].start()
    metas[2].start()
    dense_table.start()
    loads[2].wait()
    for h in range(PARTS):
        up[0][h].start()
        down[0][h].start()
    for copy in dense:
        copy.start()

    before = (iota((128, 128), 0) < iota((128, 128), 1)).astype(F32).astype(BF16)
    expert = (iota((NR, 128), 0) + z * NR).astype(F32)
    row = iota((BLK, 128), 0)
    near = row[0:NEAR]

    def spread(of, rows):
        return (of == iota((rows, NR), 1)).astype(F32).astype(BF16)

    served = iota((NEAR, NR), 0) // MAIN
    all_rows = spread(iota((BLK, NR), 0) // MAIN, BLK)
    own_rows = spread(jnp.where(served < 2, 2 * x + served, device(-s, 0) + served - 2), NEAR)
    second_rows = spread(jnp.where(served < 2, 2 * x + served, device(s, 0) + served - 2), NEAR)

    def lists(ref, j):
        named = jnp.zeros((NR, 128), F32)
        weight = jnp.zeros((NR, 128), F32)
        for k in range(8):
            hit = ref[j, k : k + 1, :] == expert
            named = jnp.where(hit, 1.0, named)
            weight = jnp.where(hit, ref[j, 8 + k : 9 + k, :], weight)
        place = jnp.where(named > 0.0, dot(named.astype(BF16), before), -1.0)
        return place.astype(BF16), weight.astype(BF16)

    def pick(mask, weight, ref, j, lo, n):
        ref[j, :, lo : lo + n] = jnp.transpose(jnp.where(mask, weight, 0.0))[0:TOK].astype(BF16)
        return jnp.where(mask, 1.0, 0.0).astype(BF16)[:, 0:TOK]

    picks, extras, own_picks, second_picks = {}, {}, {}, {}

    def selections(j):
        place, weight = lists(meta, j)
        place_j, weight_j = dot(all_rows, place), dot(all_rows, weight)
        picks[j] = pick(place_j == (row % MAIN).astype(F32), weight_j, cm, j, 0, BLK)
        extra = (place_j == (MAIN + row % 2).astype(F32)) & (row % MAIN // 2 == j)
        extras[j] = pick(extra, weight_j, cm, j, BLK, BLK)
        own_picks[j] = pick(dot(own_rows, place) == (near % MAIN).astype(F32), dot(own_rows, weight), co, j, 0, NEAR)

    def second_selections(j):
        place, weight = lists(metn, j)
        second_picks[j] = pick(
            dot(second_rows, place) == (near % MAIN).astype(F32), dot(second_rows, weight), cn, j, 0, NEAR
        )

    mine, hosted = r * MAIN, host_of * MAIN

    def send(src, dst, send_sem, recv_sem, to):
        pltpu.make_async_remote_copy(
            src_ref=src, dst_ref=dst, send_sem=send_sem, recv_sem=recv_sem, device_id=in_row(to), device_id_type=MESH
        ).start()

    def exchange(src, dst, lo, send_sem, recv_sem, col, w):
        cols = pl.ds(col, w)
        dst[tile(lo + mine), cols] = src[tile(lo + mine), cols]
        for i in range(1, NR):
            to = lax.rem(r + i, NR)
            send(src.at[tile(lo + to * MAIN), cols], dst.at[tile(lo + mine), cols], send_sem, recv_sem, to)

    def settle(rows, w, sem):
        part = rx.at[pl.ds(0, rows), pl.ds(0, w)]
        pltpu.make_async_copy(part, part, sem).wait()

    def gather(step, h, slots=None):
        for j in slots or SLOTS[step]:
            if j not in picks:
                selections(j)
            if h < FULL:
                sx[j * BLK : (j + 1) * BLK, h * COLS : (h + 1) * COLS] = dot(
                    picks[j], xz[j, :, h * COLS : (h + 1) * COLS]
                ).astype(BF16)
                exchange(sx, rx, j * BLK, xsend.at[step], xrecv.at[step], h * COLS, COLS)
            elif h < PARTS:
                serve(step, j, h, h - FULL, own_picks[j], so, mine, 0 - s)
            else:
                if h == PARTS:
                    second_selections(j)
                serve(step, j, h, h - PARTS, second_picks[j], sn, hosted, s)

    def serve(step, j, h, i, picked, src, home, far):
        cols, to_cols = pl.ds(i * COLS, COLS), pl.ds((FULL + i) * COLS, COLS)
        src[j * NEAR : (j + 1) * NEAR, cols] = dot(picked, xz[j, :, h * COLS : (h + 1) * COLS]).astype(BF16)
        dst = tile(j * BLK + home)
        rx[dst, to_cols] = src[tile(j * NEAR + c * MAIN), cols]
        for u, to in ((1 - c, 2 * x + 1 - c), (2, device(far, 0)), (3, device(far, 1))):
            send(src.at[tile(j * NEAR + u * MAIN), cols], rx.at[dst, to_cols], tsend.at[step], trecv.at[step], to)

    def gather_overflow():
        for h in range(PARTS):
            cols = slice(h * COLS, (h + 1) * COLS)
            total = dot(extras[0], xz[0, :, cols])
            for j in range(1, NZ):
                total += dot(extras[j], xz[j, :, cols])
            sx[OVF:ROWS, cols] = total.astype(BF16)
        exchange(sx, rx, OVF, osend.at[0], orecv.at[0], 0, DIM)

    def experts(step):
        first, n = SLOTS[step][0] * BLK, len(SLOTS[step]) * BLK
        settle(n // BLK * (BLK - MAIN), FULL * COLS, xrecv.at[step])
        settle(n // BLK * (BLK - 2 * MAIN), DCOLS, trecv.at[step])
        if step == 4:
            settle(BLK - MAIN, DIM, orecv.at[0])
            n += BLK

        def hidden(i, carry):
            cols = pl.ds(pl.multiple_of(i * 256, 256), 256)
            rows = rx[first : first + n, :]
            gate, upward = dot(rows, wg[:, cols]), dot(rows, wu[:, cols])
            hid[0:n, cols] = (gate / (1.0 + jnp.exp(-gate)) * upward).astype(BF16)
            return carry

        def result(i, carry):
            cols = pl.ds(pl.multiple_of(i * 256, 256), 256)
            ys[first : first + n, cols] = dot(hid[0:n, :], wd[:, cols]).astype(BF16)
            return carry

        lax.fori_loop(0, HID // 256, hidden, 0)
        lax.fori_loop(0, DIM // 256, result, 0)

    def give_back(step):
        for h in RETURNED:
            for j in SLOTS[step]:
                if h < FULL:
                    exchange(ys, yr, j * BLK, ysend.at[step, h], yrecv.at[step, h], h * COLS, COLS)
                else:
                    give_back_shared(step, j, h)
            if step == 4:
                exchange(ys, yr, OVF, psend.at[h], precv.at[h], h * COLS, COLS)

    def give_back_shared(step, j, h):
        cols, to_cols = pl.ds(h * COLS, COLS), pl.ds((h - FULL) * COLS, COLS)
        yo[tile(j * NEAR + c * MAIN), to_cols] = ys[tile(j * BLK + mine), cols]
        yn[tile(j * NEAR + c * MAIN), to_cols] = ys[tile(j * BLK + hosted), cols]
        for core, own in ((c, True), (1 - c, False)):
            way = 1 - 2 * core
            trips = [
                (device(way, core), device(way, core), yo, 2 + c),
                (device(2, core), device(-way, core), yn, 2 + c),
            ]
            if not own:
                trips += [
                    (2 * x + core, 2 * x + core, yo, c),
                    (device(-way, core), 2 * x + core, yn, c),
                ]
            for home, to, dst, u in trips:
                send(
                    ys.at[tile(j * BLK + home * MAIN), cols], dst.at[tile(j * NEAR + u * MAIN), to_cols],
                    ysend.at[step, h], yrecv.at[step, h], to,
                )

    def forward(tables, k):
        for j in SLOTS[k]:
            tables[j].wait_recv()
            if j + 2 < NZ:
                tables[j + 2].start()

    def arrive(k, slots=None):
        forward(metas, k)
        for h in range(PARTS + DUAL):
            for way in (up, down):
                way[k - 1][h].wait_recv()
                if k < 4:
                    way[k][h].start()
            if h == PARTS:
                forward(metns, k)
            gather(k, h, slots)

    for h in range(PARTS):
        gather(0, h)
    dense_table.wait_recv()
    metns[1].start()
    metns[2].start()
    for i in range(DUAL):
        dense[i].wait_recv()
        up[0][PARTS + i].start()
        down[0][PARTS + i].start()
        gather(0, PARTS + i)
    arrive(1)
    for load in loads[3:]:
        load.wait()
    experts(0)
    arrive(2)
    experts(1)
    arrive(3, (5,))
    selections(6)
    arrive(4)
    gather_overflow()
    for h in range(PARTS + DUAL):
        gather(3, h, (6,))
    experts(2)
    experts(4)
    give_back(4)
    experts(3)
    for step in (3, 2, 1, 0):
        give_back(step)

    def combine(j, h):
        i = h - FULL if h < PARTS else h - PARTS
        cols, dual_cols = slice(h * COLS, (h + 1) * COLS), slice(i * COLS, (i + 1) * COLS)
        if h >= PARTS:
            return dot(cn[j], yn[j * NEAR : (j + 1) * NEAR, dual_cols])
        extra = dot(cm[j, :, BLK : 2 * BLK], yr[OVF:ROWS, cols])
        if h >= FULL:
            return extra + dot(co[j], yo[j * NEAR : (j + 1) * NEAR, dual_cols])
        return extra + dot(cm[j, :, 0:BLK], yr[j * BLK : (j + 1) * BLK, cols])

    settled = set()

    def returned(step, h):
        h = h - DUAL if h >= PARTS else h
        if (step, h) not in settled:
            settled.add((step, h))
            if step == 4:
                settle(BLK - MAIN, COLS, precv.at[h])
            settle(len(SLOTS[step]) * (BLK - MAIN if h < FULL else BLK - 2 * MAIN), COLS, yrecv.at[step, h])

    def homeward(way, m, lo, n):
        return [
            pltpu.make_async_remote_copy(
                src_ref=zs.at[way, m, pl.ds(lo, n), pl.ds(h * COLS, COLS)],
                dst_ref=zr.at[way, m, pl.ds(lo, n), pl.ds(h * COLS, COLS)],
                send_sem=rsend.at[way, m, h], recv_sem=rrecv.at[way, m, h],
                device_id=at_z(1 - 2 * way), device_id_type=MESH,
            )
            for h in range(PARTS + DUAL)
        ]

    spans = ((0, HALF), (HALF, HALF))
    home = [[homeward(way, 0, *spans[way])] + [homeward(way, m, 0, TOK) for m in (1, 2, 3)] for way in (0, 1)]
    final = [
        pltpu.make_async_remote_copy(
            src_ref=fs.at[:, pl.ds(i * COLS, COLS)], dst_ref=fr.at[:, pl.ds(i * COLS, COLS)],
            send_sem=fsend.at[i], recv_sem=frecv.at[i], device_id=in_row(host_of), device_id_type=MESH,
        )
        for i in range(DUAL)
    ]
    def combine_step(m):
        step = 4 - m
        for h in SECOND + RETURNED:
            cols = slice(h * COLS, (h + 1) * COLS)
            returned(step, h)
            if m == 0:
                part = combine(7, h).astype(BF16)
                for way in (0, 1):
                    lo, n = spans[way]
                    zs[way, 0, lo : lo + n, cols] = part[lo : lo + n]
                    home[way][0][h].start()
                continue
            for way, j in ((0, 2 * step), (1, 2 * step - 1)):
                part = combine(j, h)
                home[way][m - 1][h].wait_recv()
                if m == 1:
                    lo, n = spans[way]
                    came = zr[way, 0, lo : lo + n, cols].astype(F32)
                    zs[way, 1, lo : lo + n, cols] = (part[lo : lo + n] + came).astype(BF16)
                    lo = HALF - lo
                    zs[way, 1, lo : lo + n, cols] = part[lo : lo + n].astype(BF16)
                else:
                    came = zr[way, m - 1, :, cols].astype(F32)
                    zs[way, m, :, cols] = (part + came).astype(BF16)
                home[way][m][h].start()

    for m in range(4):
        combine_step(m)
    for h in SECOND + tuple(range(PARTS)):
        cols = slice(h * COLS, (h + 1) * COLS)
        returned(0, h)
        total = combine(0, h)
        for way in (0, 1):
            home[way][3][h].wait_recv()
            total += zr[way, 3, :, cols].astype(F32)
        if h >= PARTS:
            i = h - PARTS
            fs[:, i * COLS : (i + 1) * COLS] = total.astype(BF16)
            final[i].start()
            continue
        if h >= FULL:
            i = h - FULL
            final[i].wait_recv()
            total += fr[:, i * COLS : (i + 1) * COLS].astype(F32)
        out[:, cols] = total.astype(BF16)

    for message in up + down + home[0] + home[1] + [dense, final, metas[1:], metns[1:], [dense_table]]:
        for copy in message:
            copy.wait_send()
    for step in range(5):
        n = len(SLOTS[step])
        settle(n * (BLK - MAIN), FULL * COLS, xsend.at[step])
        settle(n * (BLK - 2 * MAIN), DCOLS, tsend.at[step])
        for h in range(PARTS):
            settle(n * (BLK - MAIN if h < FULL else BLK - 2 * MAIN), COLS, ysend.at[step, h])
    settle(BLK - MAIN, DIM, osend.at[0])
    for h in range(PARTS):
        settle(BLK - MAIN, COLS, psend.at[h])


def local(tokens, routes, combine_weights, w_gate, w_up, w_down):
    anywhere = pl.BlockSpec(memory_space=pl.ANY)
    dma = pltpu.SemaphoreType.DMA
    return pl.pallas_call(
        kernel,
        name="routed_experts",
        out_shape=jax.ShapeDtypeStruct((TOK, DIM), BF16),
        in_specs=[anywhere] * 6,
        out_specs=pl.BlockSpec(memory_space=pltpu.VMEM),
        scratch_shapes=[
            pltpu.VMEM((NZ, TOK, WIDE), BF16),
            pltpu.VMEM((ROWS, DIM), BF16),
            pltpu.VMEM((ROWS, DIM), BF16),
            pltpu.VMEM((ROWS, DIM), BF16),
            pltpu.VMEM((ROWS, DIM), BF16),
            pltpu.VMEM((NZ * NEAR, DCOLS), BF16),
            pltpu.VMEM((NZ * NEAR, DCOLS), BF16),
            pltpu.VMEM((NZ * NEAR, DCOLS), BF16),
            pltpu.VMEM((NZ * NEAR, DCOLS), BF16),
            pltpu.VMEM((2, 4, TOK, WIDE), BF16),
            pltpu.VMEM((2, 4, TOK, WIDE), BF16),
            pltpu.VMEM((TOK, DCOLS), BF16),
            pltpu.VMEM((TOK, DCOLS), BF16),
            pltpu.VMEM((DIM, HID), BF16),
            pltpu.VMEM((DIM, HID), BF16),
            pltpu.VMEM((HID, DIM), BF16),
            pltpu.VMEM((2 * BLK, HID), BF16),
            pltpu.VMEM((TOK, 8), jnp.int32),
            pltpu.VMEM((TOK, 8), BF16),
            pltpu.VMEM((128, 128), F32),
            pltpu.VMEM((NZ, 16, 128), F32),
            pltpu.VMEM((NZ, 16, 128), F32),
            pltpu.VMEM((NZ, TOK, 2 * BLK), BF16),
            pltpu.VMEM((NZ, TOK, NEAR), BF16),
            pltpu.VMEM((NZ, TOK, NEAR), BF16),
            dma((6,)),
            dma((8, PARTS + DUAL)), dma((8, PARTS + DUAL)), dma((8,)), dma((8,)), dma((8,)), dma((8,)),
            dma((DUAL,)), dma((DUAL,)),
            dma((5,)), dma((5,)), dma((5,)), dma((5,)), dma((1,)), dma((1,)),
            dma((5, PARTS)), dma((5, PARTS)), dma((PARTS,)), dma((PARTS,)),
            dma((2, 4, PARTS + DUAL)), dma((2, 4, PARTS + DUAL)), dma((DUAL,)), dma((DUAL,)),
        ],
        compiler_params=pltpu.CompilerParams(
            collective_id=0, has_side_effects=True, vmem_limit_bytes=67_043_328
        ),
    )(tokens, routes, combine_weights, w_gate, w_up, w_down)


def solution(mesh):
    in_specs = (
        P(("dp", "ep"), None), P(("dp", "ep"), None), P(("dp", "ep"), None),
        P("ep", None, None), P("ep", None, None), P("ep", None, None),
    )
    return jax.shard_map(
        local, mesh=mesh, in_specs=in_specs, out_specs=P(("dp", "ep"), None), check_vma=False
    )
```

```python
import jax
import jax.numpy as jnp
from jax import lax
from jax.experimental import pallas as pl
from jax.experimental.pallas import tpu as pltpu
from jax.sharding import PartitionSpec as P

MESH = pl.DeviceIdType.MESH
F32, BF16 = jnp.float32, jnp.bfloat16

NZ, NX, NR = 8, 4, 8
TOK, DIM, HID = 96, 2048, 768
MAIN = 16
BLK = NR * MAIN
OVF = NZ * BLK
ROWS = OVF + BLK
HALF = TOK // 2
EARLY = 2
LIMIT = 60 * 2**20
NEAR = 4 * MAIN

PARTS, DUAL = 4, 1
FULL = PARTS - DUAL
COLS = DIM // PARTS
DCOLS = DUAL * COLS
WIDE = DIM + DCOLS
SECOND = tuple(range(PARTS, PARTS + DUAL))
RETURNED = tuple(range(FULL, PARTS)) + tuple(range(FULL))

OFFSET = (0, -1, 1, -2, 2, -3, 3, 4)
SLOTS = ((0,), (1, 2), (3, 4), (5, 6), (7,))


def dot(a, b):
    return jnp.dot(a, b, preferred_element_type=F32)


def iota(shape, axis):
    return lax.broadcasted_iota(jnp.int32, shape, axis)


def kernel(
    tokens, routes, weights, w_gate, w_up, w_down, out,
    done, xz, sx, rx, ys, yr, so, sn, yo, yn, zs, zr, fs, fr,
    wg, wu, wd, hid, listed, weighed, meta, metn, cm, co, cn,
    local_sem, zsend, zrecv, msend, mrecv, nsend, nrecv, dsend, drecv,
    xsend, xrecv, tsend, trecv, osend, orecv, ysend, yrecv, psend, precv, rsend, rrecv, fsend, frecv,
):
    me = lax.axis_index("ep")
    z, r = me // NR, me % NR
    x, c = r // 2, r % 2
    s = 1 - 2 * c

    def at_z(d):
        return {"ep": lax.rem(z + d + NZ, NZ) * NR + r}

    def in_row(other):
        return {"ep": z * NR + other}

    def device(dx, core):
        return lax.rem(x + dx + 2 * NX, NX) * 2 + core

    def tile(row):
        return pl.ds(pl.multiple_of(row, MAIN), MAIN)

    second, host_of = device(s, c), device(-s, c)
    loads = [
        pltpu.make_async_copy(routes, listed, local_sem.at[0]),
        pltpu.make_async_copy(weights, weighed, local_sem.at[1]),
        pltpu.make_async_copy(tokens, xz.at[0, :, pl.ds(0, DIM)], local_sem.at[2]),
        pltpu.make_async_copy(w_gate.at[0], wg, local_sem.at[3]),
        pltpu.make_async_copy(w_up.at[0], wu, local_sem.at[4]),
        pltpu.make_async_copy(w_down.at[0], wd, local_sem.at[5]),
    ]
    barrier = pltpu.get_barrier_semaphore()
    for d in (-1, 1):
        pl.semaphore_signal(barrier, inc=1, device_id=at_z(d), device_id_type=MESH)
    for i in range(1, NR):
        pl.semaphore_signal(barrier, inc=1, device_id=in_row(lax.rem(r + i, NR)), device_id_type=MESH)
    for load in loads:
        load.start()

    meta[0] = jnp.full((16, 128), -1.0, F32)
    loads[0].wait()
    meta[0, 0:8, 0:TOK] = listed[...].astype(F32)
    loads[1].wait()
    meta[0, 8:16, 0:TOK] = weighed[...].astype(F32)

    def ring(k, src, dst, sem, lo=0, n=TOK):
        return [
            pltpu.make_async_remote_copy(
                src_ref=xz.at[src, pl.ds(lo, n), pl.ds(h * COLS, COLS)],
                dst_ref=xz.at[dst, pl.ds(lo, n), pl.ds(h * COLS, COLS)],
                send_sem=zsend.at[sem, h], recv_sem=zrecv.at[sem, h], device_id=at_z(k), device_id_type=MESH,
            )
            for h in range(PARTS + DUAL if n == TOK else PARTS)
        ]

    def tables(ref, send, recv):
        return [None] + [
            pltpu.make_async_remote_copy(
                src_ref=ref.at[max(j - 2, 0)], dst_ref=ref.at[j], send_sem=send.at[j], recv_sem=recv.at[j],
                device_id=at_z(1 if j % 2 else -1), device_id_type=MESH,
            )
            for j in range(1, NZ)
        ]

    up = [ring(1, 0, 1, 0), ring(1, 1, 3, 2), ring(1, 3, 5, 4), ring(1, 5, 7, 6, 0, HALF)]
    down = [ring(-1, 0, 2, 1), ring(-1, 2, 4, 3), ring(-1, 4, 6, 5), ring(-1, 6, 7, 7, HALF, HALF)]
    metas, metns = tables(meta, msend, mrecv), tables(metn, nsend, nrecv)[:-1]
    dense = [
        pltpu.make_async_remote_copy(
            src_ref=xz.at[0, :, pl.ds((FULL + i) * COLS, COLS)], dst_ref=xz.at[0, :, pl.ds((PARTS + i) * COLS, COLS)],
            send_sem=dsend.at[i], recv_sem=drecv.at[i], device_id=in_row(second), device_id_type=MESH,
        )
        for i in range(DUAL)
    ]
    dense_table = pltpu.make_async_remote_copy(
        src_ref=meta.at[0], dst_ref=metn.at[0], send_sem=nsend.at[0], recv_sem=nrecv.at[0],
        device_id=in_row(second), device_id_type=MESH,
    )

    pl.semaphore_wait(barrier, 2 + NR - 1)
    metas[1].start()
    metas[2].start()
    dense_table.start()
    loads[2].wait()
    for h in range(PARTS):
        up[0][h].start()
        down[0][h].start()
    for copy in dense:
        copy.start()

    before = (iota((128, 128), 0) < iota((128, 128), 1)).astype(F32).astype(BF16)
    expert = (iota((NR, 128), 0) + z * NR).astype(F32)
    row = iota((BLK, 128), 0)
    near = row[0:NEAR]

    def spread(of, rows):
        return (of == iota((rows, NR), 1)).astype(F32).astype(BF16)

    served = iota((NEAR, NR), 0) // MAIN
    all_rows = spread(iota((BLK, NR), 0) // MAIN, BLK)
    own_rows = spread(jnp.where(served < 2, 2 * x + served, device(-s, 0) + served - 2), NEAR)
    second_rows = spread(jnp.where(served < 2, 2 * x + served, device(s, 0) + served - 2), NEAR)

    def lists(ref, j):
        named = jnp.zeros((NR, 128), F32)
        weight = jnp.zeros((NR, 128), F32)
        for k in range(8):
            hit = ref[j, k : k + 1, :] == expert
            named = jnp.where(hit, 1.0, named)
            weight = jnp.where(hit, ref[j, 8 + k : 9 + k, :], weight)
        place = jnp.where(named > 0.0, dot(named.astype(BF16), before), -1.0)
        return place.astype(BF16), weight.astype(BF16)

    def pick(mask, weight, ref, j, lo, n):
        ref[j, :, lo : lo + n] = jnp.transpose(jnp.where(mask, weight, 0.0))[0:TOK].astype(BF16)
        return jnp.where(mask, 1.0, 0.0).astype(BF16)[:, 0:TOK]

    picks, extras, own_picks, second_picks = {}, {}, {}, {}

    def selections(j):
        place, weight = lists(meta, j)
        place_j, weight_j = dot(all_rows, place), dot(all_rows, weight)
        picks[j] = pick(place_j == (row % MAIN).astype(F32), weight_j, cm, j, 0, BLK)
        extra = (place_j == (MAIN + row % 2).astype(F32)) & (row % MAIN // 2 == j)
        extras[j] = pick(extra, weight_j, cm, j, BLK, BLK)
        if j < 7:
            own_picks[j] = pick(dot(own_rows, place) == (near % MAIN).astype(F32), dot(own_rows, weight), co, j, 0, NEAR)

    def second_selections(j):
        place, weight = lists(metn, j)
        second_picks[j] = pick(
            dot(second_rows, place) == (near % MAIN).astype(F32), dot(second_rows, weight), cn, j, 0, NEAR
        )

    mine, hosted = r * MAIN, host_of * MAIN

    def send(src, dst, send_sem, recv_sem, to):
        pltpu.make_async_remote_copy(
            src_ref=src, dst_ref=dst, send_sem=send_sem, recv_sem=recv_sem, device_id=in_row(to), device_id_type=MESH
        ).start()

    def exchange(src, dst, lo, send_sem, recv_sem, col, w):
        cols = pl.ds(col, w)
        dst[tile(lo + mine), cols] = src[tile(lo + mine), cols]
        for i in range(1, NR):
            to = lax.rem(r + i, NR)
            send(src.at[tile(lo + to * MAIN), cols], dst.at[tile(lo + mine), cols], send_sem, recv_sem, to)

    def settle(rows, w, sem):
        part = rx.at[pl.ds(0, rows), pl.ds(0, w)]
        pltpu.make_async_copy(part, part, sem).wait()

    def gather(step, h, slots=None):
        for j in slots or SLOTS[step]:
            if j not in picks:
                selections(j)
            if h < FULL or (step == 4 and h < PARTS):
                sx[j * BLK : (j + 1) * BLK, h * COLS : (h + 1) * COLS] = dot(
                    picks[j], xz[j, :, h * COLS : (h + 1) * COLS]
                ).astype(BF16)
                exchange(sx, rx, j * BLK, xsend.at[step], xrecv.at[step], h * COLS, COLS)
            elif h < PARTS:
                serve(step, j, h, h - FULL, own_picks[j], so, mine, 0 - s)
            else:
                if h == PARTS:
                    second_selections(j)
                serve(step, j, h, h - PARTS, second_picks[j], sn, hosted, s)

    def serve(step, j, h, i, picked, src, home, far):
        cols, to_cols = pl.ds(i * COLS, COLS), pl.ds((FULL + i) * COLS, COLS)
        src[j * NEAR : (j + 1) * NEAR, cols] = dot(picked, xz[j, :, h * COLS : (h + 1) * COLS]).astype(BF16)
        dst = tile(j * BLK + home)
        rx[dst, to_cols] = src[tile(j * NEAR + c * MAIN), cols]
        for u, to in ((1 - c, 2 * x + 1 - c), (2, device(far, 0)), (3, device(far, 1))):
            send(src.at[tile(j * NEAR + u * MAIN), cols], rx.at[dst, to_cols], tsend.at[step], trecv.at[step], to)

    def gather_overflow():
        for h in range(PARTS):
            cols = slice(h * COLS, (h + 1) * COLS)
            total = dot(extras[0], xz[0, :, cols])
            for j in range(1, NZ):
                total += dot(extras[j], xz[j, :, cols])
            sx[OVF:ROWS, cols] = total.astype(BF16)
        exchange(sx, rx, OVF, osend.at[0], orecv.at[0], 0, DIM)

    def experts(step):
        first, n = SLOTS[step][0] * BLK, len(SLOTS[step]) * BLK
        if step == 4:
            settle(BLK - MAIN, DIM, xrecv.at[step])
            settle(BLK - MAIN, DIM, orecv.at[0])
            n += BLK
        else:
            settle(n // BLK * (BLK - MAIN), FULL * COLS, xrecv.at[step])
            settle(n // BLK * (BLK - 2 * MAIN), DCOLS, trecv.at[step])

        for i in range(0, HID, 256):
            rows = rx[first : first + n, :]
            gate, upward = dot(rows, wg[:, i : i + 256]), dot(rows, wu[:, i : i + 256])
            hid[0:n, i : i + 256] = (gate / (1.0 + jnp.exp(-gate)) * upward).astype(BF16)
        for i in range(0, DIM, 512):
            ys[first : first + n, i : i + 512] = dot(hid[0:n, :], wd[:, i : i + 512]).astype(BF16)

    def give_back(step):
        for h in RETURNED:
            for j in SLOTS[step]:
                if h < FULL or step == 4:
                    exchange(ys, yr, j * BLK, ysend.at[step, h], yrecv.at[step, h], h * COLS, COLS)
                else:
                    give_back_shared(step, j, h)
            if step == 4:
                exchange(ys, yr, OVF, psend.at[h], precv.at[h], h * COLS, COLS)

    def give_back_shared(step, j, h):
        cols, to_cols = pl.ds(h * COLS, COLS), pl.ds((h - FULL) * COLS, COLS)
        yo[tile(j * NEAR + c * MAIN), to_cols] = ys[tile(j * BLK + mine), cols]
        yn[tile(j * NEAR + c * MAIN), to_cols] = ys[tile(j * BLK + hosted), cols]
        for core, own in ((c, True), (1 - c, False)):
            way = 1 - 2 * core
            trips = [
                (device(way, core), device(way, core), yo, 2 + c),
                (device(2, core), device(-way, core), yn, 2 + c),
            ]
            if not own:
                trips += [
                    (2 * x + core, 2 * x + core, yo, c),
                    (device(-way, core), 2 * x + core, yn, c),
                ]
            for home, to, dst, u in trips:
                send(
                    ys.at[tile(j * BLK + home * MAIN), cols], dst.at[tile(j * NEAR + u * MAIN), to_cols],
                    ysend.at[step, h], yrecv.at[step, h], to,
                )

    def forward(tables, k):
        for j in SLOTS[k]:
            tables[j].wait_recv()
            if j + 2 < len(tables):
                tables[j + 2].start()

    def arrive(k, slots=None, early=0):
        forward(metas, k)
        for h in range(PARTS):
            pass_on(k, h)
            gather(k, h, SLOTS[k] if h < early else slots)

    def pass_on(k, h):
        for way in (up, down):
            way[k - 1][h].wait_recv()
            if k < (4 if h < PARTS else 3):
                way[k][h].start()

    def arrive_second(k, slots=None):
        forward(metns, k)
        for h in SECOND:
            pass_on(k, h)
            gather(k, h, slots)

    for h in range(PARTS):
        gather(0, h)
    dense_table.wait_recv()
    metns[1].start()
    metns[2].start()
    for i in range(DUAL):
        dense[i].wait_recv()
        gather(0, PARTS + i)
    arrive(1)
    for h in SECOND:
        up[0][h].start()
        down[0][h].start()
    for load in loads[3:]:
        load.wait()
    experts(0)
    arrive(2)
    arrive_second(1)
    arrive(3, (5,), EARLY)
    arrive_second(2)
    arrive(4)
    gather_overflow()
    for h in range(EARLY, PARTS):
        gather(3, h, (6,))
    arrive_second(3)
    experts(1)
    experts(2)
    experts(4)
    give_back(4)
    experts(3)
    for step in (3, 2, 1, 0):
        give_back(step)

    def combine(j, h):
        i = h - FULL if h < PARTS else h - PARTS
        cols, dual_cols = slice(h * COLS, (h + 1) * COLS), slice(i * COLS, (i + 1) * COLS)
        if h >= PARTS:
            return dot(cn[j], yn[j * NEAR : (j + 1) * NEAR, dual_cols])
        extra = dot(cm[j, :, BLK : 2 * BLK], yr[OVF:ROWS, cols])
        if h >= FULL and j < 7:
            return extra + dot(co[j], yo[j * NEAR : (j + 1) * NEAR, dual_cols])
        return extra + dot(cm[j, :, 0:BLK], yr[j * BLK : (j + 1) * BLK, cols])

    settled = set()

    def returned(step, h):
        h = h - DUAL if h >= PARTS else h
        if (step, h) not in settled:
            settled.add((step, h))
            if step == 4:
                settle(BLK - MAIN, COLS, precv.at[h])
            settle(len(SLOTS[step]) * (BLK - MAIN if h < FULL or step == 4 else BLK - 2 * MAIN), COLS, yrecv.at[step, h])

    def homeward(way, m, lo, n):
        return [
            pltpu.make_async_remote_copy(
                src_ref=zs.at[way, m, pl.ds(lo, n), pl.ds(h * COLS, COLS)],
                dst_ref=zr.at[way, m, pl.ds(lo, n), pl.ds(h * COLS, COLS)],
                send_sem=rsend.at[way, m, h], recv_sem=rrecv.at[way, m, h],
                device_id=at_z(1 - 2 * way), device_id_type=MESH,
            )
            for h in range(PARTS + DUAL if m else PARTS)
        ]

    spans = ((0, HALF), (HALF, HALF))
    home = [[homeward(way, 0, *spans[way])] + [homeward(way, m, 0, TOK) for m in (1, 2, 3)] for way in (0, 1)]
    final = [
        pltpu.make_async_remote_copy(
            src_ref=fs.at[:, pl.ds(i * COLS, COLS)], dst_ref=fr.at[:, pl.ds(i * COLS, COLS)],
            send_sem=fsend.at[i], recv_sem=frecv.at[i], device_id=in_row(host_of), device_id_type=MESH,
        )
        for i in range(DUAL)
    ]
    def combine_step(m):
        step = 4 - m
        for h in (SECOND if m else ()) + RETURNED:
            cols = slice(h * COLS, (h + 1) * COLS)
            returned(step, h)
            if m == 0:
                part = combine(7, h).astype(BF16)
                for way in (0, 1):
                    lo, n = spans[way]
                    zs[way, 0, lo : lo + n, cols] = part[lo : lo + n]
                    home[way][0][h].start()
                continue
            for way, j in ((0, 2 * step), (1, 2 * step - 1)):
                part = combine(j, h)
                if m == 1 and h >= PARTS:
                    zs[way, 1, :, cols] = part.astype(BF16)
                    home[way][1][h].start()
                    continue
                home[way][m - 1][h].wait_recv()
                if m == 1:
                    lo, n = spans[way]
                    came = zr[way, 0, lo : lo + n, cols].astype(F32)
                    zs[way, 1, lo : lo + n, cols] = (part[lo : lo + n] + came).astype(BF16)
                    lo = HALF - lo
                    zs[way, 1, lo : lo + n, cols] = part[lo : lo + n].astype(BF16)
                else:
                    came = zr[way, m - 1, :, cols].astype(F32)
                    zs[way, m, :, cols] = (part + came).astype(BF16)
                home[way][m][h].start()

    for m in range(4):
        combine_step(m)
    stores = []
    for h in SECOND + tuple(range(PARTS)):
        cols = slice(h * COLS, (h + 1) * COLS)
        returned(0, h)
        total = combine(0, h)
        for way in (0, 1):
            home[way][3][h].wait_recv()
            total += zr[way, 3, :, cols].astype(F32)
        if h >= PARTS:
            i = h - PARTS
            fs[:, i * COLS : (i + 1) * COLS] = total.astype(BF16)
            final[i].start()
            continue
        if h >= FULL:
            i = h - FULL
            final[i].wait_recv()
            total += fr[:, i * COLS : (i + 1) * COLS].astype(F32)
        done[:, cols] = total.astype(BF16)
        stores.append(pltpu.make_async_copy(done.at[:, cols], out.at[:, cols], local_sem.at[6 + h]))
        stores[-1].start()

    for message in up + down + home[0] + home[1] + [dense, final, metas[1:], metns[1:], [dense_table]]:
        for copy in message:
            copy.wait_send()
    for step in range(5):
        n = len(SLOTS[step])
        settle(n * (BLK - MAIN), DIM if step == 4 else FULL * COLS, xsend.at[step])
        if step < 4:
            settle(n * (BLK - 2 * MAIN), DCOLS, tsend.at[step])
        for h in range(PARTS):
            settle(n * (BLK - MAIN if h < FULL or step == 4 else BLK - 2 * MAIN), COLS, ysend.at[step, h])
    for store in stores:
        store.wait()
    settle(BLK - MAIN, DIM, osend.at[0])
    for h in range(PARTS):
        settle(BLK - MAIN, COLS, psend.at[h])


def local(tokens, routes, combine_weights, w_gate, w_up, w_down):
    in_hbm = pl.BlockSpec(memory_space=pltpu.HBM)
    dma = pltpu.SemaphoreType.DMA
    return pl.pallas_call(
        kernel,
        name="routed_experts",
        out_shape=jax.ShapeDtypeStruct((TOK, DIM), BF16),
        in_specs=[in_hbm] * 6,
        out_specs=in_hbm,
        scratch_shapes=[
            pltpu.VMEM((TOK, DIM), BF16),
            pltpu.VMEM((NZ, TOK, WIDE), BF16),
            pltpu.VMEM((ROWS, DIM), BF16),
            pltpu.VMEM((ROWS, DIM), BF16),
            pltpu.VMEM((ROWS, DIM), BF16),
            pltpu.VMEM((ROWS, DIM), BF16),
            pltpu.VMEM((NZ * NEAR, DCOLS), BF16),
            pltpu.VMEM((NZ * NEAR, DCOLS), BF16),
            pltpu.VMEM((NZ * NEAR, DCOLS), BF16),
            pltpu.VMEM((NZ * NEAR, DCOLS), BF16),
            pltpu.VMEM((2, 4, TOK, WIDE), BF16),
            pltpu.VMEM((2, 4, TOK, WIDE), BF16),
            pltpu.VMEM((TOK, DCOLS), BF16),
            pltpu.VMEM((TOK, DCOLS), BF16),
            pltpu.VMEM((DIM, HID), BF16),
            pltpu.VMEM((DIM, HID), BF16),
            pltpu.VMEM((HID, DIM), BF16),
            pltpu.VMEM((2 * BLK, HID), BF16),
            pltpu.VMEM((8, TOK), jnp.int32),
            pltpu.VMEM((8, TOK), BF16),
            pltpu.VMEM((NZ, 16, 128), F32),
            pltpu.VMEM((NZ, 16, 128), F32),
            pltpu.VMEM((NZ, TOK, 2 * BLK), BF16),
            pltpu.VMEM((NZ, TOK, NEAR), BF16),
            pltpu.VMEM((NZ, TOK, NEAR), BF16),
            dma((6 + PARTS,)),
            dma((8, PARTS + DUAL)), dma((8, PARTS + DUAL)), dma((8,)), dma((8,)), dma((8,)), dma((8,)),
            dma((DUAL,)), dma((DUAL,)),
            dma((5,)), dma((5,)), dma((5,)), dma((5,)), dma((1,)), dma((1,)),
            dma((5, PARTS)), dma((5, PARTS)), dma((PARTS,)), dma((PARTS,)),
            dma((2, 4, PARTS + DUAL)), dma((2, 4, PARTS + DUAL)), dma((DUAL,)), dma((DUAL,)),
        ],
        compiler_params=pltpu.CompilerParams(
            collective_id=0, has_side_effects=True, vmem_limit_bytes=LIMIT
        ),
    )(tokens, routes.T, combine_weights.T, w_gate, w_up, w_down)


def solution(mesh):
    in_specs = (
        P(("dp", "ep"), None), P(("dp", "ep"), None), P(("dp", "ep"), None),
        P("ep", None, None), P("ep", None, None), P("ep", None, None),
    )
    return jax.shard_map(
        local, mesh=mesh, in_specs=in_specs, out_specs=P(("dp", "ep"), None), check_vma=False
    )
```

```python
import jax
import jax.numpy as jnp
from jax import lax
from jax.experimental import pallas as pl
from jax.experimental.pallas import tpu as pltpu
from jax.sharding import PartitionSpec as P

MESH = pl.DeviceIdType.MESH
F32, BF16 = jnp.float32, jnp.bfloat16

NZ, NX, NR = 8, 4, 8
TOK, DIM, HID = 96, 2048, 768
MAIN = 16
BLK = NR * MAIN
OVF = NZ * BLK
ROWS = OVF + BLK
HALF = TOK // 2
EARLY = 2
LIMIT = 50 * 2**20
NEAR = 4 * MAIN

PARTS, DUAL = 4, 1
FULL = PARTS - DUAL
COLS = DIM // PARTS
DCOLS = DUAL * COLS
WIDE = DIM + DCOLS
SECOND = tuple(range(PARTS, PARTS + DUAL))
RETURNED = tuple(range(FULL, PARTS)) + tuple(range(FULL))

OFFSET = (0, -1, 1, -2, 2, -3, 3, 4)
SLOTS = ((0,), (1, 2), (3, 4), (5, 6), (7,))


def dot(a, b):
    return jnp.dot(a, b, preferred_element_type=F32)


def iota(shape, axis):
    return lax.broadcasted_iota(jnp.int32, shape, axis)


def kernel(
    tokens, routes, weights, w_gate, w_up, w_down, out,
    xz, sx, rx, ys, yr, so, sn, yo, yn, zs, zr, fs, fr,
    wg, wu, wd, hid, listed, weighed, meta, metn, cm, co, cn,
    local_sem, zsend, zrecv, msend, mrecv, nsend, nrecv, dsend, drecv,
    xsend, xrecv, tsend, trecv, osend, orecv, ysend, yrecv, psend, precv, rsend, rrecv, fsend, frecv,
):
    me = lax.axis_index("ep")
    z, r = me // NR, me % NR
    x, c = r // 2, r % 2
    s = 1 - 2 * c

    def at_z(d):
        return {"ep": lax.rem(z + d + NZ, NZ) * NR + r}

    def in_row(other):
        return {"ep": z * NR + other}

    def device(dx, core):
        return lax.rem(x + dx + 2 * NX, NX) * 2 + core

    def tile(row):
        return pl.ds(pl.multiple_of(row, MAIN), MAIN)

    second, host_of = device(s, c), device(-s, c)
    loads = [
        pltpu.make_async_copy(routes, listed, local_sem.at[0]),
        pltpu.make_async_copy(weights, weighed, local_sem.at[1]),
        pltpu.make_async_copy(tokens, xz.at[0, :, pl.ds(0, DIM)], local_sem.at[2]),
        pltpu.make_async_copy(w_gate.at[0], wg, local_sem.at[3]),
        pltpu.make_async_copy(w_up.at[0], wu, local_sem.at[4]),
        pltpu.make_async_copy(w_down.at[0], wd, local_sem.at[5]),
    ]
    barrier = pltpu.get_barrier_semaphore()
    for d in (-1, 1):
        pl.semaphore_signal(barrier, inc=1, device_id=at_z(d), device_id_type=MESH)
    for i in range(1, NR):
        pl.semaphore_signal(barrier, inc=1, device_id=in_row(lax.rem(r + i, NR)), device_id_type=MESH)
    for load in loads:
        load.start()

    meta[0] = jnp.full((16, 128), -1.0, F32)
    loads[0].wait()
    meta[0, 0:8, 0:TOK] = listed[...].astype(F32)
    loads[1].wait()
    meta[0, 8:16, 0:TOK] = weighed[...].astype(F32)

    def ring(k, src, dst, sem, lo=0, n=TOK):
        return [
            pltpu.make_async_remote_copy(
                src_ref=xz.at[src, pl.ds(lo, n), pl.ds(h * COLS, COLS)],
                dst_ref=xz.at[dst, pl.ds(lo, n), pl.ds(h * COLS, COLS)],
                send_sem=zsend.at[sem, h], recv_sem=zrecv.at[sem, h], device_id=at_z(k), device_id_type=MESH,
            )
            for h in range(PARTS + DUAL if n == TOK else PARTS)
        ]

    def tables(ref, send, recv):
        return [None] + [
            pltpu.make_async_remote_copy(
                src_ref=ref.at[max(j - 2, 0)], dst_ref=ref.at[j], send_sem=send.at[j], recv_sem=recv.at[j],
                device_id=at_z(1 if j % 2 else -1), device_id_type=MESH,
            )
            for j in range(1, NZ)
        ]

    up = [ring(1, 0, 1, 0), ring(1, 1, 3, 2), ring(1, 3, 5, 4), ring(1, 5, 7, 6, 0, HALF)]
    down = [ring(-1, 0, 2, 1), ring(-1, 2, 4, 3), ring(-1, 4, 6, 5), ring(-1, 6, 7, 7, HALF, HALF)]
    metas, metns = tables(meta, msend, mrecv), tables(metn, nsend, nrecv)[:-1]
    dense = [
        pltpu.make_async_remote_copy(
            src_ref=xz.at[0, :, pl.ds((FULL + i) * COLS, COLS)], dst_ref=xz.at[0, :, pl.ds((PARTS + i) * COLS, COLS)],
            send_sem=dsend.at[i], recv_sem=drecv.at[i], device_id=in_row(second), device_id_type=MESH,
        )
        for i in range(DUAL)
    ]
    dense_table = pltpu.make_async_remote_copy(
        src_ref=meta.at[0], dst_ref=metn.at[0], send_sem=nsend.at[0], recv_sem=nrecv.at[0],
        device_id=in_row(second), device_id_type=MESH,
    )

    pl.semaphore_wait(barrier, 2 + NR - 1)
    metas[1].start()
    metas[2].start()
    dense_table.start()
    loads[2].wait()
    for h in range(PARTS):
        up[0][h].start()
        down[0][h].start()
    for copy in dense:
        copy.start()

    before = (iota((128, 128), 0) < iota((128, 128), 1)).astype(F32).astype(BF16)
    expert = (iota((NR, 128), 0) + z * NR).astype(F32)
    row = iota((BLK, 128), 0)
    near = row[0:NEAR]

    def spread(of, rows):
        return (of == iota((rows, NR), 1)).astype(F32).astype(BF16)

    served = iota((NEAR, NR), 0) // MAIN
    all_rows = spread(iota((BLK, NR), 0) // MAIN, BLK)
    own_rows = spread(jnp.where(served < 2, 2 * x + served, device(-s, 0) + served - 2), NEAR)
    second_rows = spread(jnp.where(served < 2, 2 * x + served, device(s, 0) + served - 2), NEAR)

    def lists(ref, j):
        named = jnp.zeros((NR, 128), F32)
        weight = jnp.zeros((NR, 128), F32)
        for k in range(8):
            hit = ref[j, k : k + 1, :] == expert
            named = jnp.where(hit, 1.0, named)
            weight = jnp.where(hit, ref[j, 8 + k : 9 + k, :], weight)
        place = jnp.where(named > 0.0, dot(named.astype(BF16), before), -1.0)
        return place.astype(BF16), weight.astype(BF16)

    def pick(mask, weight, ref, j, lo, n):
        ref[j, :, lo : lo + n] = jnp.transpose(jnp.where(mask, weight, 0.0))[0:TOK].astype(BF16)
        return jnp.where(mask, 1.0, 0.0).astype(BF16)[:, 0:TOK]

    picks, extras, own_picks, second_picks = {}, {}, {}, {}

    def selections(j):
        place, weight = lists(meta, j)
        place_j, weight_j = dot(all_rows, place), dot(all_rows, weight)
        picks[j] = pick(place_j == (row % MAIN).astype(F32), weight_j, cm, j, 0, BLK)
        extra = (place_j == (MAIN + row % 2).astype(F32)) & (row % MAIN // 2 == j)
        extras[j] = pick(extra, weight_j, cm, j, BLK, BLK)
        if j < 7:
            own_picks[j] = pick(dot(own_rows, place) == (near % MAIN).astype(F32), dot(own_rows, weight), co, j, 0, NEAR)

    def second_selections(j):
        place, weight = lists(metn, j)
        second_picks[j] = pick(
            dot(second_rows, place) == (near % MAIN).astype(F32), dot(second_rows, weight), cn, j, 0, NEAR
        )

    mine, hosted = r * MAIN, host_of * MAIN

    def send(src, dst, send_sem, recv_sem, to):
        pltpu.make_async_remote_copy(
            src_ref=src, dst_ref=dst, send_sem=send_sem, recv_sem=recv_sem, device_id=in_row(to), device_id_type=MESH
        ).start()

    def exchange(src, dst, lo, send_sem, recv_sem, col, w):
        cols = pl.ds(col, w)
        dst[tile(lo + mine), cols] = src[tile(lo + mine), cols]
        for i in range(1, NR):
            to = lax.rem(r + i, NR)
            send(src.at[tile(lo + to * MAIN), cols], dst.at[tile(lo + mine), cols], send_sem, recv_sem, to)

    def settle(rows, w, sem):
        part = rx.at[pl.ds(0, rows), pl.ds(0, w)]
        pltpu.make_async_copy(part, part, sem).wait()

    def gather(step, h, slots=None):
        for j in slots or SLOTS[step]:
            if j not in picks:
                selections(j)
            if h < FULL or (step == 4 and h < PARTS):
                sx[j * BLK : (j + 1) * BLK, h * COLS : (h + 1) * COLS] = dot(
                    picks[j], xz[j, :, h * COLS : (h + 1) * COLS]
                ).astype(BF16)
                exchange(sx, rx, j * BLK, xsend.at[step], xrecv.at[step], h * COLS, COLS)
            elif h < PARTS:
                serve(step, j, h, h - FULL, own_picks[j], so, mine, 0 - s)
            else:
                if h == PARTS:
                    second_selections(j)
                serve(step, j, h, h - PARTS, second_picks[j], sn, hosted, s)

    def serve(step, j, h, i, picked, src, home, far):
        cols, to_cols = pl.ds(i * COLS, COLS), pl.ds((FULL + i) * COLS, COLS)
        src[j * NEAR : (j + 1) * NEAR, cols] = dot(picked, xz[j, :, h * COLS : (h + 1) * COLS]).astype(BF16)
        dst = tile(j * BLK + home)
        rx[dst, to_cols] = src[tile(j * NEAR + c * MAIN), cols]
        for u, to in ((1 - c, 2 * x + 1 - c), (2, device(far, 0)), (3, device(far, 1))):
            send(src.at[tile(j * NEAR + u * MAIN), cols], rx.at[dst, to_cols], tsend.at[step], trecv.at[step], to)

    def gather_overflow():
        for h in range(PARTS):
            cols = slice(h * COLS, (h + 1) * COLS)
            total = dot(extras[0], xz[0, :, cols])
            for j in range(1, NZ):
                total += dot(extras[j], xz[j, :, cols])
            sx[OVF:ROWS, cols] = total.astype(BF16)
        exchange(sx, rx, OVF, osend.at[0], orecv.at[0], 0, DIM)

    def experts(step, then=None):
        first, n = SLOTS[step][0] * BLK, len(SLOTS[step]) * BLK
        if step == 4:
            settle(BLK - MAIN, DIM, xrecv.at[step])
            settle(BLK - MAIN, DIM, orecv.at[0])
            n += BLK
        else:
            settle(n // BLK * (BLK - MAIN), FULL * COLS, xrecv.at[step])
            settle(n // BLK * (BLK - 2 * MAIN), DCOLS, trecv.at[step])

        for i in range(0, HID, 256):
            rows = rx[first : first + n, :]
            gate, upward = dot(rows, wg[:, i : i + 256]), dot(rows, wu[:, i : i + 256])
            hid[0:n, i : i + 256] = (gate / (1.0 + jnp.exp(-gate)) * upward).astype(BF16)
        for h in RETURNED:
            cols = slice(h * COLS, (h + 1) * COLS)
            ys[first : first + n, cols] = dot(hid[0:n, :], wd[:, cols]).astype(BF16)
            if then:
                then(step, h)

    def give_back(step, h):
        for j in SLOTS[step]:
            if h < FULL or step == 4:
                exchange(ys, yr, j * BLK, ysend.at[step, h], yrecv.at[step, h], h * COLS, COLS)
            else:
                give_back_shared(step, j, h)
        if step == 4:
            exchange(ys, yr, OVF, psend.at[h], precv.at[h], h * COLS, COLS)

    def give_back_shared(step, j, h):
        cols, to_cols = pl.ds(h * COLS, COLS), pl.ds((h - FULL) * COLS, COLS)
        yo[tile(j * NEAR + c * MAIN), to_cols] = ys[tile(j * BLK + mine), cols]
        yn[tile(j * NEAR + c * MAIN), to_cols] = ys[tile(j * BLK + hosted), cols]
        for core, own in ((c, True), (1 - c, False)):
            way = 1 - 2 * core
            trips = [
                (device(way, core), device(way, core), yo, 2 + c),
                (device(2, core), device(-way, core), yn, 2 + c),
            ]
            if not own:
                trips += [
                    (2 * x + core, 2 * x + core, yo, c),
                    (device(-way, core), 2 * x + core, yn, c),
                ]
            for home, to, dst, u in trips:
                send(
                    ys.at[tile(j * BLK + home * MAIN), cols], dst.at[tile(j * NEAR + u * MAIN), to_cols],
                    ysend.at[step, h], yrecv.at[step, h], to,
                )

    def forward(tables, k):
        for j in SLOTS[k]:
            tables[j].wait_recv()
            if j + 2 < len(tables):
                tables[j + 2].start()

    def arrive(k, slots=None, early=0):
        forward(metas, k)
        for h in range(PARTS):
            pass_on(k, h)
            gather(k, h, SLOTS[k] if h < early else slots)

    def pass_on(k, h):
        for way in (up, down):
            way[k - 1][h].wait_recv()
            if k < (4 if h < PARTS else 3):
                way[k][h].start()

    def arrive_second(k, slots=None):
        forward(metns, k)
        for h in SECOND:
            pass_on(k, h)
            gather(k, h, slots)

    for h in range(PARTS):
        gather(0, h)
    dense_table.wait_recv()
    metns[1].start()
    metns[2].start()
    for i in range(DUAL):
        dense[i].wait_recv()
        gather(0, PARTS + i)
    arrive(1)
    for h in SECOND:
        up[0][h].start()
        down[0][h].start()
    for load in loads[3:]:
        load.wait()
    experts(0)
    arrive(2)
    arrive_second(1)
    arrive(3, (5,), EARLY)
    arrive_second(2)
    arrive(4)
    gather_overflow()
    for h in range(EARLY, PARTS):
        gather(3, h, (6,))
    arrive_second(3)
    experts(1)
    experts(2)
    experts(4, give_back)
    experts(3, give_back)
    for step in (2, 1, 0):
        for h in RETURNED:
            give_back(step, h)

    def combine(j, h):
        i = h - FULL if h < PARTS else h - PARTS
        cols, dual_cols = slice(h * COLS, (h + 1) * COLS), slice(i * COLS, (i + 1) * COLS)
        if h >= PARTS:
            return dot(cn[j], yn[j * NEAR : (j + 1) * NEAR, dual_cols])
        extra = dot(cm[j, :, BLK : 2 * BLK], yr[OVF:ROWS, cols])
        if h >= FULL and j < 7:
            return extra + dot(co[j], yo[j * NEAR : (j + 1) * NEAR, dual_cols])
        return extra + dot(cm[j, :, 0:BLK], yr[j * BLK : (j + 1) * BLK, cols])

    settled = set()

    def returned(step, h):
        h = h - DUAL if h >= PARTS else h
        if (step, h) not in settled:
            settled.add((step, h))
            if step == 4:
                settle(BLK - MAIN, COLS, precv.at[h])
            settle(len(SLOTS[step]) * (BLK - MAIN if h < FULL or step == 4 else BLK - 2 * MAIN), COLS, yrecv.at[step, h])

    def homeward(way, m, lo, n):
        return [
            pltpu.make_async_remote_copy(
                src_ref=zs.at[way, m, pl.ds(lo, n), pl.ds(h * COLS, COLS)],
                dst_ref=zr.at[way, m, pl.ds(lo, n), pl.ds(h * COLS, COLS)],
                send_sem=rsend.at[way, m, h], recv_sem=rrecv.at[way, m, h],
                device_id=at_z(1 - 2 * way), device_id_type=MESH,
            )
            for h in range(PARTS + DUAL if m else PARTS)
        ]

    spans = ((0, HALF), (HALF, HALF))
    home = [[homeward(way, 0, *spans[way])] + [homeward(way, m, 0, TOK) for m in (1, 2, 3)] for way in (0, 1)]
    final = [
        pltpu.make_async_remote_copy(
            src_ref=fs.at[:, pl.ds(i * COLS, COLS)], dst_ref=fr.at[:, pl.ds(i * COLS, COLS)],
            send_sem=fsend.at[i], recv_sem=frecv.at[i], device_id=in_row(host_of), device_id_type=MESH,
        )
        for i in range(DUAL)
    ]
    def combine_step(m):
        step = 4 - m
        for h in (SECOND if m else ()) + RETURNED:
            cols = slice(h * COLS, (h + 1) * COLS)
            returned(step, h)
            if m == 0:
                part = combine(7, h).astype(BF16)
                for way in (0, 1):
                    lo, n = spans[way]
                    zs[way, 0, lo : lo + n, cols] = part[lo : lo + n]
                    home[way][0][h].start()
                continue
            for way, j in ((0, 2 * step), (1, 2 * step - 1)):
                part = combine(j, h)
                if m == 1 and h >= PARTS:
                    zs[way, 1, :, cols] = part.astype(BF16)
                    home[way][1][h].start()
                    continue
                home[way][m - 1][h].wait_recv()
                if m == 1:
                    lo, n = spans[way]
                    came = zr[way, 0, lo : lo + n, cols].astype(F32)
                    zs[way, 1, lo : lo + n, cols] = (part[lo : lo + n] + came).astype(BF16)
                    lo = HALF - lo
                    zs[way, 1, lo : lo + n, cols] = part[lo : lo + n].astype(BF16)
                else:
                    came = zr[way, m - 1, :, cols].astype(F32)
                    zs[way, m, :, cols] = (part + came).astype(BF16)
                home[way][m][h].start()

    for m in range(4):
        combine_step(m)
    for h in SECOND + tuple(range(PARTS)):
        cols = slice(h * COLS, (h + 1) * COLS)
        returned(0, h)
        total = combine(0, h)
        for way in (0, 1):
            home[way][3][h].wait_recv()
            total += zr[way, 3, :, cols].astype(F32)
        if h >= PARTS:
            i = h - PARTS
            fs[:, i * COLS : (i + 1) * COLS] = total.astype(BF16)
            final[i].start()
            continue
        if h >= FULL:
            i = h - FULL
            final[i].wait_recv()
            total += fr[:, i * COLS : (i + 1) * COLS].astype(F32)
        out[:, cols] = total.astype(BF16)

    for message in up + down + home[0] + home[1] + [dense, final, metas[1:], metns[1:], [dense_table]]:
        for copy in message:
            copy.wait_send()
    for step in range(5):
        n = len(SLOTS[step])
        settle(n * (BLK - MAIN), DIM if step == 4 else FULL * COLS, xsend.at[step])
        if step < 4:
            settle(n * (BLK - 2 * MAIN), DCOLS, tsend.at[step])
        for h in range(PARTS):
            settle(n * (BLK - MAIN if h < FULL or step == 4 else BLK - 2 * MAIN), COLS, ysend.at[step, h])
    settle(BLK - MAIN, DIM, osend.at[0])
    for h in range(PARTS):
        settle(BLK - MAIN, COLS, psend.at[h])


def hold(a):
    return pltpu.with_memory_space_constraint(a, pltpu.HBM)


def local(tokens, routes, combine_weights, w_gate, w_up, w_down):
    in_hbm = pl.BlockSpec(memory_space=pltpu.HBM)
    dma = pltpu.SemaphoreType.DMA
    return pl.pallas_call(
        kernel,
        name="routed_experts",
        out_shape=jax.ShapeDtypeStruct((TOK, DIM), BF16),
        in_specs=[in_hbm] * 6,
        out_specs=pl.BlockSpec(memory_space=pltpu.VMEM),
        scratch_shapes=[
            pltpu.VMEM((NZ, TOK, WIDE), BF16),
            pltpu.VMEM((ROWS, DIM), BF16),
            pltpu.VMEM((ROWS, DIM), BF16),
            pltpu.VMEM((ROWS, DIM), BF16),
            pltpu.VMEM((ROWS, DIM), BF16),
            pltpu.VMEM((NZ * NEAR, DCOLS), BF16),
            pltpu.VMEM((NZ * NEAR, DCOLS), BF16),
            pltpu.VMEM((NZ * NEAR, DCOLS), BF16),
            pltpu.VMEM((NZ * NEAR, DCOLS), BF16),
            pltpu.VMEM((2, 4, TOK, WIDE), BF16),
            pltpu.VMEM((2, 4, TOK, WIDE), BF16),
            pltpu.VMEM((TOK, DCOLS), BF16),
            pltpu.VMEM((TOK, DCOLS), BF16),
            pltpu.VMEM((DIM, HID), BF16),
            pltpu.VMEM((DIM, HID), BF16),
            pltpu.VMEM((HID, DIM), BF16),
            pltpu.VMEM((2 * BLK, HID), BF16),
            pltpu.VMEM((8, TOK), jnp.int32),
            pltpu.VMEM((8, TOK), BF16),
            pltpu.VMEM((NZ, 16, 128), F32),
            pltpu.VMEM((NZ, 16, 128), F32),
            pltpu.VMEM((NZ, TOK, 2 * BLK), BF16),
            pltpu.VMEM((NZ, TOK, NEAR), BF16),
            pltpu.VMEM((NZ, TOK, NEAR), BF16),
            dma((6,)),
            dma((8, PARTS + DUAL)), dma((8, PARTS + DUAL)), dma((8,)), dma((8,)), dma((8,)), dma((8,)),
            dma((DUAL,)), dma((DUAL,)),
            dma((5,)), dma((5,)), dma((5,)), dma((5,)), dma((1,)), dma((1,)),
            dma((5, PARTS)), dma((5, PARTS)), dma((PARTS,)), dma((PARTS,)),
            dma((2, 4, PARTS + DUAL)), dma((2, 4, PARTS + DUAL)), dma((DUAL,)), dma((DUAL,)),
        ],
        compiler_params=pltpu.CompilerParams(
            collective_id=0, has_side_effects=True, vmem_limit_bytes=LIMIT
        ),
    )(*(hold(a) for a in (tokens, routes.T, combine_weights.T, w_gate, w_up, w_down)))


def solution(mesh):
    in_specs = (
        P(("dp", "ep"), None), P(("dp", "ep"), None), P(("dp", "ep"), None),
        P("ep", None, None), P("ep", None, None), P("ep", None, None),
    )
    return jax.shard_map(
        local, mesh=mesh, in_specs=in_specs, out_specs=P(("dp", "ep"), None), check_vma=False
    )
```

```python
import jax
import jax.numpy as jnp
from jax import lax
from jax.experimental import pallas as pl
from jax.experimental.pallas import tpu as pltpu
from jax.sharding import PartitionSpec as P

MESH = pl.DeviceIdType.MESH
F32, BF16 = jnp.float32, jnp.bfloat16

NZ, NX, NR = 8, 4, 8
TOK, DIM, HID = 96, 2048, 768
MAIN = 16
BLK = NR * MAIN
OVF = NZ * BLK
ROWS = OVF + BLK
HALF = TOK // 2
EARLY = 2
LIMIT = 50 * 2**20
NEAR = 4 * MAIN

PARTS, DUAL = 4, 1
FULL = PARTS - DUAL
COLS = DIM // PARTS
DCOLS = DUAL * COLS
WIDE = DIM + DCOLS
SECOND = tuple(range(PARTS, PARTS + DUAL))
RETURNED = tuple(range(FULL, PARTS)) + tuple(range(FULL))

OFFSET = (0, -1, 1, -2, 2, -3, 3, 4)
SLOTS = ((0,), (1, 2), (3, 4), (5, 6), (7,))


def dot(a, b):
    return jnp.dot(a, b, preferred_element_type=F32)


def iota(shape, axis):
    return lax.broadcasted_iota(jnp.int32, shape, axis)


def kernel(
    tokens, routes, weights, w_gate, w_up, w_down, out,
    xz, sx, rx, ys, yr, so, sn, yo, yn, zs, zr, fs, fr,
    wg, wu, wd, hid, listed, weighed, meta, metn, cm, co, cn,
    local_sem, zsend, zrecv, msend, mrecv, nsend, nrecv, dsend, drecv,
    xsend, xrecv, tsend, trecv, osend, orecv, ysend, yrecv, psend, precv, rsend, rrecv, fsend, frecv,
):
    me = lax.axis_index("ep")
    z, r = me // NR, me % NR
    x, c = r // 2, r % 2
    s = 1 - 2 * c

    def at_z(d):
        return {"ep": lax.rem(z + d + NZ, NZ) * NR + r}

    def in_row(other):
        return {"ep": z * NR + other}

    def device(dx, core):
        return lax.rem(x + dx + 2 * NX, NX) * 2 + core

    def tile(row):
        return pl.ds(pl.multiple_of(row, MAIN), MAIN)

    second, host_of = device(s, c), device(-s, c)
    loads = [
        pltpu.make_async_copy(routes, listed, local_sem.at[0]),
        pltpu.make_async_copy(weights, weighed, local_sem.at[1]),
        pltpu.make_async_copy(tokens, xz.at[0, :, pl.ds(0, DIM)], local_sem.at[2]),
        pltpu.make_async_copy(w_gate.at[0], wg, local_sem.at[3]),
        pltpu.make_async_copy(w_up.at[0], wu, local_sem.at[4]),
        pltpu.make_async_copy(w_down.at[0], wd, local_sem.at[5]),
    ]
    barrier = pltpu.get_barrier_semaphore()
    for d in (-1, 1):
        pl.semaphore_signal(barrier, inc=1, device_id=at_z(d), device_id_type=MESH)
    for i in range(1, NR):
        pl.semaphore_signal(barrier, inc=1, device_id=in_row(lax.rem(r + i, NR)), device_id_type=MESH)
    for load in loads:
        load.start()

    meta[0] = jnp.full((16, 128), -1.0, F32)
    loads[0].wait()
    meta[0, 0:8, 0:TOK] = listed[...].astype(F32)
    loads[1].wait()
    meta[0, 8:16, 0:TOK] = weighed[...].astype(F32)

    def ring(k, src, dst, sem, lo=0, n=TOK):
        return [
            pltpu.make_async_remote_copy(
                src_ref=xz.at[src, pl.ds(lo, n), pl.ds(h * COLS, COLS)],
                dst_ref=xz.at[dst, pl.ds(lo, n), pl.ds(h * COLS, COLS)],
                send_sem=zsend.at[sem, h], recv_sem=zrecv.at[sem, h], device_id=at_z(k), device_id_type=MESH,
            )
            for h in range(PARTS + DUAL if n == TOK else PARTS)
        ]

    def tables(ref, send, recv):
        return [None] + [
            pltpu.make_async_remote_copy(
                src_ref=ref.at[max(j - 2, 0)], dst_ref=ref.at[j], send_sem=send.at[j], recv_sem=recv.at[j],
                device_id=at_z(1 if j % 2 else -1), device_id_type=MESH,
            )
            for j in range(1, NZ)
        ]

    up = [ring(1, 0, 1, 0), ring(1, 1, 3, 2), ring(1, 3, 5, 4), ring(1, 5, 7, 6, 0, HALF)]
    down = [ring(-1, 0, 2, 1), ring(-1, 2, 4, 3), ring(-1, 4, 6, 5), ring(-1, 6, 7, 7, HALF, HALF)]
    metas, metns = tables(meta, msend, mrecv), tables(metn, nsend, nrecv)[:-1]
    dense = [
        pltpu.make_async_remote_copy(
            src_ref=xz.at[0, :, pl.ds((FULL + i) * COLS, COLS)], dst_ref=xz.at[0, :, pl.ds((PARTS + i) * COLS, COLS)],
            send_sem=dsend.at[i], recv_sem=drecv.at[i], device_id=in_row(second), device_id_type=MESH,
        )
        for i in range(DUAL)
    ]
    dense_table = pltpu.make_async_remote_copy(
        src_ref=meta.at[0], dst_ref=metn.at[0], send_sem=nsend.at[0], recv_sem=nrecv.at[0],
        device_id=in_row(second), device_id_type=MESH,
    )

    pl.semaphore_wait(barrier, 2 + NR - 1)
    metas[1].start()
    metas[2].start()
    dense_table.start()
    loads[2].wait()
    for h in range(PARTS):
        up[0][h].start()
        down[0][h].start()
    for copy in dense:
        copy.start()

    before = (iota((128, 128), 0) < iota((128, 128), 1)).astype(F32).astype(BF16)
    expert = (iota((NR, 128), 0) + z * NR).astype(F32)
    row = iota((BLK, 128), 0)
    near = row[0:NEAR]

    def spread(of, rows):
        return (of == iota((rows, NR), 1)).astype(F32).astype(BF16)

    served = iota((NEAR, NR), 0) // MAIN
    all_rows = spread(iota((BLK, NR), 0) // MAIN, BLK)
    own_rows = spread(jnp.where(served < 2, 2 * x + served, device(-s, 0) + served - 2), NEAR)
    second_rows = spread(jnp.where(served < 2, 2 * x + served, device(s, 0) + served - 2), NEAR)

    def lists(ref, j):
        named = jnp.zeros((NR, 128), F32)
        weight = jnp.zeros((NR, 128), F32)
        for k in range(8):
            hit = ref[j, k : k + 1, :] == expert
            named = jnp.where(hit, 1.0, named)
            weight = jnp.where(hit, ref[j, 8 + k : 9 + k, :], weight)
        place = jnp.where(named > 0.0, dot(named.astype(BF16), before), -1.0)
        return place.astype(BF16), weight.astype(BF16)

    def pick(mask, weight, ref, j, lo, n):
        ref[j, :, lo : lo + n] = jnp.transpose(jnp.where(mask, weight, 0.0))[0:TOK].astype(BF16)
        return jnp.where(mask, 1.0, 0.0).astype(BF16)[:, 0:TOK]

    picks, extras, own_picks, second_picks = {}, {}, {}, {}

    def selections(j):
        place, weight = lists(meta, j)
        place_j, weight_j = dot(all_rows, place), dot(all_rows, weight)
        picks[j] = pick(place_j == (row % MAIN).astype(F32), weight_j, cm, j, 0, BLK)
        extra = (place_j == (MAIN + row % 2).astype(F32)) & (row % MAIN // 2 == j)
        extras[j] = pick(extra, weight_j, cm, j, BLK, BLK)
        if j < 7:
            own_picks[j] = pick(dot(own_rows, place) == (near % MAIN).astype(F32), dot(own_rows, weight), co, j, 0, NEAR)

    def second_selections(j):
        place, weight = lists(metn, j)
        second_picks[j] = pick(
            dot(second_rows, place) == (near % MAIN).astype(F32), dot(second_rows, weight), cn, j, 0, NEAR
        )

    mine, hosted = r * MAIN, host_of * MAIN

    def send(src, dst, send_sem, recv_sem, to):
        pltpu.make_async_remote_copy(
            src_ref=src, dst_ref=dst, send_sem=send_sem, recv_sem=recv_sem, device_id=in_row(to), device_id_type=MESH
        ).start()

    def exchange(src, dst, lo, send_sem, recv_sem, col, w):
        cols = pl.ds(col, w)
        dst[tile(lo + mine), cols] = src[tile(lo + mine), cols]
        for i in range(1, NR):
            to = lax.rem(r + i, NR)
            send(src.at[tile(lo + to * MAIN), cols], dst.at[tile(lo + mine), cols], send_sem, recv_sem, to)

    def settle(rows, w, sem):
        part = rx.at[pl.ds(0, rows), pl.ds(0, w)]
        pltpu.make_async_copy(part, part, sem).wait()

    def gather(step, h, slots=None):
        for j in slots or SLOTS[step]:
            if j not in picks:
                selections(j)
            if h < FULL or (step == 4 and h < PARTS):
                sx[j * BLK : (j + 1) * BLK, h * COLS : (h + 1) * COLS] = dot(
                    picks[j], xz[j, :, h * COLS : (h + 1) * COLS]
                ).astype(BF16)
                exchange(sx, rx, j * BLK, xsend.at[step], xrecv.at[step], h * COLS, COLS)
            elif h < PARTS:
                serve(step, j, h, h - FULL, own_picks[j], so, mine, 0 - s)
            else:
                if h == PARTS:
                    second_selections(j)
                serve(step, j, h, h - PARTS, second_picks[j], sn, hosted, s)

    def serve(step, j, h, i, picked, src, home, far):
        cols, to_cols = pl.ds(i * COLS, COLS), pl.ds((FULL + i) * COLS, COLS)
        src[j * NEAR : (j + 1) * NEAR, cols] = dot(picked, xz[j, :, h * COLS : (h + 1) * COLS]).astype(BF16)
        dst = tile(j * BLK + home)
        rx[dst, to_cols] = src[tile(j * NEAR + c * MAIN), cols]
        for u, to in ((1 - c, 2 * x + 1 - c), (2, device(far, 0)), (3, device(far, 1))):
            send(src.at[tile(j * NEAR + u * MAIN), cols], rx.at[dst, to_cols], tsend.at[step], trecv.at[step], to)

    def gather_overflow():
        for h in range(PARTS):
            cols = slice(h * COLS, (h + 1) * COLS)
            total = dot(extras[0], xz[0, :, cols])
            for j in range(1, NZ):
                total += dot(extras[j], xz[j, :, cols])
            sx[OVF:ROWS, cols] = total.astype(BF16)
        exchange(sx, rx, OVF, osend.at[0], orecv.at[0], 0, DIM)

    def experts(step, then=None):
        first, n = SLOTS[step][0] * BLK, len(SLOTS[step]) * BLK
        if step == 4:
            settle(BLK - MAIN, DIM, xrecv.at[step])
            settle(BLK - MAIN, DIM, orecv.at[0])
            n += BLK
        else:
            settle(n // BLK * (BLK - MAIN), FULL * COLS, xrecv.at[step])
            settle(n // BLK * (BLK - 2 * MAIN), DCOLS, trecv.at[step])

        for i in range(0, HID, 256):
            rows = rx[first : first + n, :]
            gate, upward = dot(rows, wg[:, i : i + 256]), dot(rows, wu[:, i : i + 256])
            hid[0:n, i : i + 256] = (gate / (1.0 + jnp.exp(-gate)) * upward).astype(BF16)
        for h in RETURNED:
            cols = slice(h * COLS, (h + 1) * COLS)
            ys[first : first + n, cols] = dot(hid[0:n, :], wd[:, cols]).astype(BF16)
            if then:
                then(step, h)

    def give_back(step, h):
        for j in SLOTS[step]:
            if h < FULL or step > 2:
                exchange(ys, yr, j * BLK, ysend.at[step, h], yrecv.at[step, h], h * COLS, COLS)
            else:
                give_back_shared(step, j, h)
        if step == 4:
            exchange(ys, yr, OVF, psend.at[h], precv.at[h], h * COLS, COLS)

    def give_back_shared(step, j, h):
        cols, to_cols = pl.ds(h * COLS, COLS), pl.ds((h - FULL) * COLS, COLS)
        yo[tile(j * NEAR + c * MAIN), to_cols] = ys[tile(j * BLK + mine), cols]
        yn[tile(j * NEAR + c * MAIN), to_cols] = ys[tile(j * BLK + hosted), cols]
        for core, own in ((c, True), (1 - c, False)):
            way = 1 - 2 * core
            trips = [
                (device(way, core), device(way, core), yo, 2 + c),
                (device(2, core), device(-way, core), yn, 2 + c),
            ]
            if not own:
                trips += [
                    (2 * x + core, 2 * x + core, yo, c),
                    (device(-way, core), 2 * x + core, yn, c),
                ]
            for home, to, dst, u in trips:
                send(
                    ys.at[tile(j * BLK + home * MAIN), cols], dst.at[tile(j * NEAR + u * MAIN), to_cols],
                    ysend.at[step, h], yrecv.at[step, h], to,
                )

    def forward(tables, k):
        for j in SLOTS[k]:
            tables[j].wait_recv()
            if j + 2 < len(tables):
                tables[j + 2].start()

    def arrive(k, slots=None, early=0):
        forward(metas, k)
        for h in range(PARTS):
            pass_on(k, h)
            gather(k, h, SLOTS[k] if h < early else slots)

    def pass_on(k, h):
        for way in (up, down):
            way[k - 1][h].wait_recv()
            if k < (4 if h < PARTS else 3):
                way[k][h].start()

    def arrive_second(k, slots=None):
        forward(metns, k)
        for h in SECOND:
            pass_on(k, h)
            gather(k, h, slots)

    for h in range(PARTS):
        gather(0, h)
    dense_table.wait_recv()
    metns[1].start()
    metns[2].start()
    for i in range(DUAL):
        dense[i].wait_recv()
        gather(0, PARTS + i)
    arrive(1)
    for h in SECOND:
        up[0][h].start()
        down[0][h].start()
    for load in loads[3:]:
        load.wait()
    experts(0)
    arrive(2)
    arrive_second(1)
    arrive(3, (5,), EARLY)
    arrive_second(2)
    arrive(4)
    gather_overflow()
    for h in range(EARLY, PARTS):
        gather(3, h, (6,))
    arrive_second(3)
    experts(1)
    experts(2)
    for step in (2, 1, 0):
        for h in range(FULL, PARTS):
            give_back(step, h)
    experts(4, give_back)
    experts(3, give_back)
    for step in (2, 1, 0):
        for h in range(FULL):
            give_back(step, h)

    def combine(j, h):
        i = h - FULL if h < PARTS else h - PARTS
        cols, dual_cols = slice(h * COLS, (h + 1) * COLS), slice(i * COLS, (i + 1) * COLS)
        if h >= PARTS:
            return dot(cn[j], yn[j * NEAR : (j + 1) * NEAR, dual_cols])
        extra = dot(cm[j, :, BLK : 2 * BLK], yr[OVF:ROWS, cols])
        if h >= FULL and j < 5:
            return extra + dot(co[j], yo[j * NEAR : (j + 1) * NEAR, dual_cols])
        return extra + dot(cm[j, :, 0:BLK], yr[j * BLK : (j + 1) * BLK, cols])

    settled = set()

    def returned(step, h):
        h = h - DUAL if h >= PARTS else h
        if (step, h) not in settled:
            settled.add((step, h))
            if step == 4:
                settle(BLK - MAIN, COLS, precv.at[h])
            settle(len(SLOTS[step]) * (BLK - MAIN if h < FULL or step > 2 else BLK - 2 * MAIN), COLS, yrecv.at[step, h])

    def homeward(way, m, lo, n):
        return [
            pltpu.make_async_remote_copy(
                src_ref=zs.at[way, m, pl.ds(lo, n), pl.ds(h * COLS, COLS)],
                dst_ref=zr.at[way, m, pl.ds(lo, n), pl.ds(h * COLS, COLS)],
                send_sem=rsend.at[way, m, h], recv_sem=rrecv.at[way, m, h],
                device_id=at_z(1 - 2 * way), device_id_type=MESH,
            )
            for h in range(PARTS + DUAL if m > 1 else PARTS)
        ]

    spans = ((0, HALF), (HALF, HALF))
    home = [[homeward(way, 0, *spans[way])] + [homeward(way, m, 0, TOK) for m in (1, 2, 3)] for way in (0, 1)]
    final = [
        pltpu.make_async_remote_copy(
            src_ref=fs.at[:, pl.ds(i * COLS, COLS)], dst_ref=fr.at[:, pl.ds(i * COLS, COLS)],
            send_sem=fsend.at[i], recv_sem=frecv.at[i], device_id=in_row(host_of), device_id_type=MESH,
        )
        for i in range(DUAL)
    ]
    def combine_step(m):
        step = 4 - m
        for h in RETURNED:
            cols = slice(h * COLS, (h + 1) * COLS)
            returned(step, h)
            if m == 0:
                part = combine(7, h).astype(BF16)
                for way in (0, 1):
                    lo, n = spans[way]
                    zs[way, 0, lo : lo + n, cols] = part[lo : lo + n]
                    home[way][0][h].start()
                continue
            for way, j in ((0, 2 * step), (1, 2 * step - 1)):
                part = combine(j, h)
                home[way][m - 1][h].wait_recv()
                if m == 1:
                    lo, n = spans[way]
                    came = zr[way, 0, lo : lo + n, cols].astype(F32)
                    zs[way, 1, lo : lo + n, cols] = (part[lo : lo + n] + came).astype(BF16)
                    lo = HALF - lo
                    zs[way, 1, lo : lo + n, cols] = part[lo : lo + n].astype(BF16)
                else:
                    came = zr[way, m - 1, :, cols].astype(F32)
                    zs[way, m, :, cols] = (part + came).astype(BF16)
                home[way][m][h].start()

    def second_step(m):
        step = 4 - m
        for h in SECOND:
            i = h - PARTS
            cols = slice(h * COLS, (h + 1) * COLS)
            returned(step, h)
            if m == 4:
                total = combine(0, h)
                for way in (0, 1):
                    home[way][3][h].wait_recv()
                    total += zr[way, 3, :, cols].astype(F32)
                fs[:, i * COLS : (i + 1) * COLS] = total.astype(BF16)
                final[i].start()
                continue
            for way, j in ((0, 2 * step), (1, 2 * step - 1)):
                part = combine(j, h)
                if m == 3:
                    home[way][2][h].wait_recv()
                    part += zr[way, 2, :, cols].astype(F32)
                zs[way, m, :, cols] = part.astype(BF16)
                home[way][m][h].start()

    for m in range(4):
        if m < 3:
            second_step(m + 2)
        combine_step(m)
    for h in range(PARTS):
        cols = slice(h * COLS, (h + 1) * COLS)
        returned(0, h)
        total = combine(0, h)
        for way in (0, 1):
            home[way][3][h].wait_recv()
            total += zr[way, 3, :, cols].astype(F32)
        if h >= FULL:
            i = h - FULL
            final[i].wait_recv()
            total += fr[:, i * COLS : (i + 1) * COLS].astype(F32)
        out[:, cols] = total.astype(BF16)

    for message in up + down + home[0] + home[1] + [dense, final, metas[1:], metns[1:], [dense_table]]:
        for copy in message:
            copy.wait_send()
    for step in range(5):
        n = len(SLOTS[step])
        settle(n * (BLK - MAIN), DIM if step == 4 else FULL * COLS, xsend.at[step])
        if step < 4:
            settle(n * (BLK - 2 * MAIN), DCOLS, tsend.at[step])
        for h in range(PARTS):
            settle(n * (BLK - MAIN if h < FULL or step > 2 else BLK - 2 * MAIN), COLS, ysend.at[step, h])
    settle(BLK - MAIN, DIM, osend.at[0])
    for h in range(PARTS):
        settle(BLK - MAIN, COLS, psend.at[h])


def hold(a):
    return pltpu.with_memory_space_constraint(a, pltpu.HBM)


def local(tokens, routes, combine_weights, w_gate, w_up, w_down):
    in_hbm = pl.BlockSpec(memory_space=pltpu.HBM)
    dma = pltpu.SemaphoreType.DMA
    return pl.pallas_call(
        kernel,
        name="routed_experts",
        out_shape=jax.ShapeDtypeStruct((TOK, DIM), BF16),
        in_specs=[in_hbm] * 6,
        out_specs=pl.BlockSpec(memory_space=pltpu.VMEM),
        scratch_shapes=[
            pltpu.VMEM((NZ, TOK, WIDE), BF16),
            pltpu.VMEM((ROWS, DIM), BF16),
            pltpu.VMEM((ROWS, DIM), BF16),
            pltpu.VMEM((ROWS, DIM), BF16),
            pltpu.VMEM((ROWS, DIM), BF16),
            pltpu.VMEM((NZ * NEAR, DCOLS), BF16),
            pltpu.VMEM((NZ * NEAR, DCOLS), BF16),
            pltpu.VMEM((NZ * NEAR, DCOLS), BF16),
            pltpu.VMEM((NZ * NEAR, DCOLS), BF16),
            pltpu.VMEM((2, 4, TOK, WIDE), BF16),
            pltpu.VMEM((2, 4, TOK, WIDE), BF16),
            pltpu.VMEM((TOK, DCOLS), BF16),
            pltpu.VMEM((TOK, DCOLS), BF16),
            pltpu.VMEM((DIM, HID), BF16),
            pltpu.VMEM((DIM, HID), BF16),
            pltpu.VMEM((HID, DIM), BF16),
            pltpu.VMEM((2 * BLK, HID), BF16),
            pltpu.VMEM((8, TOK), jnp.int32),
            pltpu.VMEM((8, TOK), BF16),
            pltpu.VMEM((NZ, 16, 128), F32),
            pltpu.VMEM((NZ, 16, 128), F32),
            pltpu.VMEM((NZ, TOK, 2 * BLK), BF16),
            pltpu.VMEM((NZ, TOK, NEAR), BF16),
            pltpu.VMEM((NZ, TOK, NEAR), BF16),
            dma((6,)),
            dma((8, PARTS + DUAL)), dma((8, PARTS + DUAL)), dma((8,)), dma((8,)), dma((8,)), dma((8,)),
            dma((DUAL,)), dma((DUAL,)),
            dma((5,)), dma((5,)), dma((5,)), dma((5,)), dma((1,)), dma((1,)),
            dma((5, PARTS)), dma((5, PARTS)), dma((PARTS,)), dma((PARTS,)),
            dma((2, 4, PARTS + DUAL)), dma((2, 4, PARTS + DUAL)), dma((DUAL,)), dma((DUAL,)),
        ],
        compiler_params=pltpu.CompilerParams(
            collective_id=0, has_side_effects=True, vmem_limit_bytes=LIMIT
        ),
    )(*(hold(a) for a in (tokens, routes.T, combine_weights.T, w_gate, w_up, w_down)))


def solution(mesh):
    in_specs = (
        P(("dp", "ep"), None), P(("dp", "ep"), None), P(("dp", "ep"), None),
        P("ep", None, None), P("ep", None, None), P("ep", None, None),
    )
    return jax.shard_map(
        local, mesh=mesh, in_specs=in_specs, out_specs=P(("dp", "ep"), None), check_vma=False
    )
```
